32 devices in a mesh: site: 16 (over z, x, core), sec: 2 (over y).
Axes of the slice: x: 2, y: 2, z: 4, core: 2. Of those that a mesh axis runs over, the one named last changes fastest.
Arguments:
- left_canon: bfloat16 [16, 4, 4, 128, 128], P('site', None, 'sec'), may hold values from -1.5 to 1.5
- right_canon: bfloat16 [16, 4, 4, 128, 128], P('site', None, 'sec'), may hold values from -1.5 to 1.5
- center_site: bfloat16 [16, 4, 4, 128, 128], P('site', None, 'sec'), may hold values from -6 to 6
- center_bond: bfloat16 [16, 4, 128, 128], P('site', 'sec'), may hold values from -2 to 3
- left_seed: bfloat16 [16, 4, 128, 128], P('site', 'sec'), may hold values from -2 to 4
- right_seed: bfloat16 [16, 4, 128, 128], P('site', 'sec'), may hold values from -2 to 4
- left_sector: int32 [16, 4, 4], P('site'), may hold values from 0 to 3, each once within a row
- onsite: float32 [16, 4], P('site'), may hold values from 0.5 to 2
- bond_shift: float32 [16], P('site'), may hold values from 0.5 to 2
Outputs:
- left_new: bfloat16 [16, 4, 4, 128, 128], P('site', None, 'sec')
- right_new: bfloat16 [16, 4, 4, 128, 128], P('site', None, 'sec')
The draws below stay inside these ranges and needn't reach their ends.
Inputs may be any that keep to these rules, and one draw needn't show every extreme that they name: `left_sector`: for each site and local state the 4 entries are a permutation of the sectors.
All inputs are finite; a program needn't handle non-finite values.
Results may differ from the reference program's by a relative error of at most 0.028.
Values may be sent and summed in bfloat16 or wider, within the bound.
A program may use at most 64 MiB of HBM per device.

```python
import math
import jax
import jax.numpy as jnp
from jax import lax

B = 128
PHYS = 4
NSI = 10
NAPP = 2
SITES = 16
NSEC = 4
RCH = 4


def noise_shaped(key, shape):
    values = jnp.clip(jax.random.normal(key, shape, jnp.float32), -4.0, 4.0)
    return values


def noise_field(key):
    return noise_shaped(key, (SITES, NSEC, B, B))


def canon_tensor(key):
    values = noise_shaped(jax.random.fold_in(key, 3), (SITES, PHYS, NSEC, B, B))
    leading = jax.random.randint(jax.random.fold_in(key, 5), (SITES,), 0, PHYS)
    states = jnp.arange(PHYS, dtype=jnp.int32)
    weights = jnp.where(states[None, :] == leading[:, None], 0.9, 0.2).astype(jnp.float32)
    identity = jnp.eye(B, dtype=jnp.float32)
    return (weights[:, :, None, None, None] * identity + 0.25 / math.sqrt(B) * values).astype(jnp.bfloat16)


def symmetric_seed(key):
    values = noise_field(jax.random.fold_in(key, 1))
    mixed = (values + jnp.swapaxes(values, -1, -2)) * 0.70710678
    levels = jnp.exp(jax.random.uniform(jax.random.fold_in(key, 2), (SITES, NSEC), jnp.float32, math.log(0.5), math.log(2.0)))
    blocks = jnp.eye(B, dtype=jnp.float32) + 0.5 / math.sqrt(B) * mixed
    return (levels[:, :, None, None] * blocks).astype(jnp.bfloat16)


def draw_left_canon(key, part):
    return canon_tensor(jax.random.fold_in(key, 41))


def draw_right_canon(key, part):
    return canon_tensor(jax.random.fold_in(key, 53))


def draw_center_bond(key, part):
    values = noise_field(jax.random.fold_in(key, 11))
    return (jnp.eye(B, dtype=jnp.float32) + 0.3 / math.sqrt(B) * values).astype(jnp.bfloat16)


def draw_left_seed(key, part):
    return symmetric_seed(jax.random.fold_in(key, 23))


def draw_right_seed(key, part):
    return symmetric_seed(jax.random.fold_in(key, 37))


def shard_levels(key, dims, shards, smallest, largest):
    gain, own = 1.0, jax.random.fold_in(key, 6)
    for position, shards_of in shards:
        draws = jnp.exp(jax.random.uniform(jax.random.fold_in(own, position), (shards_of,), jnp.float32, smallest / len(shards), largest / len(shards)))
        gain = gain * jnp.repeat(draws, dims[position] // shards_of).reshape([-1 if axis == position else 1 for axis in range(len(dims))])
    return gain


def bell_draw(own_key, shape, width, bound, pieces=(), kind=jnp.bfloat16):
    drawn = jax.random.normal(own_key, shape, jnp.float32) * width
    if len(pieces) > 0:
        drawn = shard_levels(own_key, shape, pieces, -0.22, 0.18) * drawn
    return jnp.clip(drawn, min=-bound, max=bound).astype(kind)


def setup_inputs(seed: int = 0) -> dict:
    keys = jax.random.split(jax.random.key(seed), 10)
    left_canon = draw_left_canon(jax.random.fold_in(keys[9], 71), 0)
    right_canon = draw_right_canon(jax.random.fold_in(keys[9], 71), 0)
    center_site = bell_draw(keys[2], (SITES, PHYS, NSEC, B, B), 1.0, 6.0, ((0, 16), (2, 2)))
    center_bond = draw_center_bond(jax.random.fold_in(keys[9], 71), 0)
    left_seed = draw_left_seed(jax.random.fold_in(keys[9], 71), 0)
    right_seed = draw_right_seed(jax.random.fold_in(keys[9], 71), 0)
    left_sector = jax.vmap(lambda own: jax.random.permutation(own, NSEC))(jax.random.split(keys[6], SITES * PHYS)).reshape((SITES, PHYS, NSEC)).astype(jnp.int32)
    onsite = jnp.clip(jnp.exp(math.log(2.0) - 1.3862944 * jax.random.uniform(keys[7], (SITES, PHYS), jnp.float32) ** shard_levels(keys[7], (SITES, PHYS), ((0, 16),), -0.2, 0.2)), 0.5, 2.0)
    bond_shift = jnp.clip(jnp.exp(math.log(2.0) - 1.3862944 * jax.random.uniform(keys[8], (SITES,), jnp.float32) ** shard_levels(keys[8], (SITES,), ((0, 16),), -0.2, 0.2)), 0.5, 2.0)
    return {"left_canon": left_canon, "right_canon": right_canon, "center_site": center_site, "center_bond": center_bond, "left_seed": left_seed, "right_seed": right_seed, "left_sector": left_sector, "onsite": onsite, "bond_shift": bond_shift}


def pick_blocks(blocks, indices):
    return jax.vmap(lambda chosen, where_at: jnp.take(chosen, where_at, axis=0))(blocks, indices)

def inverse_root(gram_mat):
    scaling = jnp.sqrt(lax.optimization_barrier(jnp.sum(gram_mat * gram_mat, axis=(-2, -1), keepdims=True)))
    identity = jnp.eye(gram_mat.shape[-1], dtype=jnp.float32)
    upper_part = gram_mat / scaling
    lower_part = jnp.broadcast_to(identity, gram_mat.shape)
    for repeat in range(NSI):
        middle = 1.5 * identity - 0.5 * jnp.matmul(lower_part, upper_part, precision=lax.Precision.HIGHEST)
        upper_part = jnp.matmul(upper_part, middle, precision=lax.Precision.HIGHEST)
        lower_part = jnp.matmul(middle, lower_part, precision=lax.Precision.HIGHEST)
    return lower_part / jnp.sqrt(scaling)

def trace_sum(blocks):
    return lax.optimization_barrier(jnp.sum(jnp.diagonal(blocks.astype(jnp.float32), axis1=2, axis2=3), axis=(1, 2)))

def reference(left_canon, right_canon, center_site, center_bond, left_seed, right_seed, left_sector, onsite, bond_shift):
    labels = jnp.arange(NSEC, dtype=jnp.int32)
    right_of = lax.optimization_barrier(jnp.sum(jnp.where(left_sector[:, :, :, None] == labels[None, None, None, :], labels[None, None, :, None], 0), axis=2)).astype(jnp.int32)
    routing = (left_sector[:, :, :, None] == labels[None, None, None, :]).astype(jnp.float32)

    def left_step(hold):
        running = jnp.zeros(hold.shape, jnp.float32)
        for physical in range(PHYS):
            tensor = left_canon[:, physical].astype(jnp.float32)
            chosen = pick_blocks(hold, left_sector[:, physical]).astype(jnp.float32)
            product = jnp.einsum('jkab,jkbc->jkac', chosen, tensor).astype(jnp.bfloat16)
            running = running + jnp.einsum('jkba,jkbc->jkac', tensor, product.astype(jnp.float32))
        return running.astype(jnp.bfloat16)

    def right_step(hold):
        running = jnp.zeros(hold.shape, jnp.float32)
        for physical in range(PHYS):
            picked = pick_blocks(right_canon[:, physical], right_of[:, physical]).astype(jnp.float32)
            env_chosen = pick_blocks(hold, right_of[:, physical]).astype(jnp.float32)
            product = jnp.einsum('jkab,jkbc->jkac', picked, env_chosen).astype(jnp.bfloat16)
            running = running + jnp.einsum('jkac,jkdc->jkad', product.astype(jnp.float32), picked)
        return running.astype(jnp.bfloat16)
    left_hold = left_seed
    right_hold = right_seed
    left_fresh = left_seed
    for step in range(RCH):
        left_fresh = left_step(left_hold)
        right_fresh = right_step(right_hold)
        left_hold = jnp.roll(left_fresh, 1, axis=0)
        right_hold = jnp.roll(right_fresh, -1, axis=0)
    dim_all = NSEC * B

    def scaled(blocks):
        return (blocks.astype(jnp.float32) * (dim_all / trace_sum(blocks))[:, None, None, None]).astype(jnp.bfloat16)
    cur_scaled = scaled(left_hold)
    next_scaled = scaled(left_fresh)
    right_scaled = scaled(right_hold)
    chosen_left = pick_blocks(cur_scaled, left_sector).astype(jnp.float32)
    site_now = center_site
    bond_now = center_bond
    for repeat in range(NAPP):
        half_site = jnp.einsum('jskab,jskbc->jskac', chosen_left, site_now.astype(jnp.float32)).astype(jnp.bfloat16)
        site_now = (jnp.einsum('jskab,jkbc->jskac', half_site.astype(jnp.float32), right_scaled.astype(jnp.float32)) + onsite[:, :, None, None, None] * site_now.astype(jnp.float32)).astype(jnp.bfloat16)
        half_bond = jnp.einsum('jkab,jkbc->jkac', next_scaled.astype(jnp.float32), bond_now.astype(jnp.float32)).astype(jnp.bfloat16)
        bond_now = (jnp.einsum('jkab,jkbc->jkac', half_bond.astype(jnp.float32), right_scaled.astype(jnp.float32)) + bond_shift[:, None, None, None] * bond_now.astype(jnp.float32)).astype(jnp.bfloat16)
    site_wide = site_now.astype(jnp.float32)
    bond_wide = bond_now.astype(jnp.float32)
    gram_left = jnp.einsum('jskab,jskac->jkbc', site_wide, site_wide)
    gram_bond = jnp.einsum('jkab,jkac->jkbc', bond_wide, bond_wide)
    unit_left = jnp.matmul(bond_wide, inverse_root(gram_bond), precision=lax.Precision.HIGHEST)
    factor_left = jnp.matmul(inverse_root(gram_left), jnp.swapaxes(unit_left, -1, -2), precision=lax.Precision.HIGHEST).astype(jnp.bfloat16)
    left_new = jnp.einsum('jskab,jkbc->jskac', site_wide, factor_left.astype(jnp.float32)).astype(jnp.bfloat16)
    outer_terms = jnp.einsum('jskab,jskcb->jskac', site_wide, site_wide)
    gram_right = jnp.einsum('jskm,jskac->jmac', routing, outer_terms)
    previous = jnp.roll(bond_now, 1, axis=0).astype(jnp.float32)
    gram_prev = jnp.matmul(previous, jnp.swapaxes(previous, -1, -2), precision=lax.Precision.HIGHEST)
    unit_right = jnp.matmul(inverse_root(gram_prev), previous, precision=lax.Precision.HIGHEST)
    factor_right = jnp.matmul(jnp.swapaxes(unit_right, -1, -2), inverse_root(gram_right), precision=lax.Precision.HIGHEST).astype(jnp.bfloat16)
    factor_chosen = pick_blocks(factor_right, left_sector).astype(jnp.float32)
    right_new = jnp.einsum('jskab,jskbc->jskac', factor_chosen, site_wide).astype(jnp.bfloat16)
    return (left_new, right_new)
```

```python
import functools

import jax
import jax.numpy as jnp
from jax import lax
from jax.experimental import pallas as pl
from jax.experimental.pallas import tpu as pltpu
from jax.sharding import PartitionSpec as P

NSI = 10
NAPP = 2
EARLY = 3
VMEM_BYTES = 67043328
RESERVED = 10240 * 1024
SLACK = 44 * 1024
MESH = pl.DeviceIdType.MESH
F32 = jnp.float32
BF16 = jnp.bfloat16


def dot(a, b):
    return lax.dot_general(a, b, (((1,), (0,)), ((), ())), preferred_element_type=F32)


def dot_nt(a, b):
    return lax.dot_general(a, b, (((1,), (1,)), ((), ())), preferred_element_type=F32)


def dot_tn(a, b):
    return lax.dot_general(a, b, (((0,), (0,)), ((), ())), preferred_element_type=F32)


def split(x):
    hi = x.astype(BF16)
    return hi, (x - hi.astype(F32)).astype(BF16)


def beside(pair):
    return jnp.concatenate(pair, axis=1)


def below(pair):
    return jnp.concatenate(pair, axis=0)


def twice_wide(x):
    return beside((x, x))


def twice_tall(x):
    return below((x, x))


def kernel(
    steps, sites, parts, phys, owned,
    lc_in, rc_in, cs_in, cb_in, lseed_in, rseed_in, src, onsite, shift,
    *refs,
):
    blocks = phys * owned
    left_new, right_new = refs[:blocks], refs[blocks : 2 * blocks]
    (
    lc, rc, cs, cb, lseed, rseed, site, fall,
    hold_l, lrecv, lsend, rrecv, psend, terms, lct, bond, ys, zs, env_r,
    gsend, grecv, usend, urecv, tns, tnr, trs, trr,
    s_in, s_ls, s_lr, s_ps, s_pr, s_gs, s_gr, s_us, s_ur, s_tns, s_tnr, s_trs, s_trr,
    ) = refs[2 * blocks :]
    j = lax.axis_index("site")
    me = lax.axis_index("sec")
    after, before = lax.rem(j + 1, sites), lax.rem(j + sites - 1, sites)
    off = me * owned
    width = lc.shape[-1]
    sectors = parts * owned
    pairs = sectors // 2

    def load(i, a, b):
        return pltpu.make_async_copy(a, b, s_in.at[i])

    loads = [
        load(0, lseed_in, lseed), load(1, rseed_in, rseed), load(2, rc_in, rc),
        load(3, lc_in, lc), load(4, cb_in, cb), load(5, cs_in, cs),
    ]
    for c in loads:
        c.start()

    def sec(d):
        return lax.rem(me + d, parts)

    def copy(a, b, ss, rs, to_site, to_sec):
        return pltpu.make_async_remote_copy(
            src_ref=a, dst_ref=b, send_sem=ss, recv_sem=rs,
            device_id={"site": to_site, "sec": to_sec}, device_id_type=MESH,
        )

    def c_seed(d):
        return copy(lseed.at[0], lrecv.at[0, me], s_ls.at[steps, d], s_lr.at[0, me], j, sec(d))

    def c_left(t, d):
        return copy(lsend.at[t], lrecv.at[t + 1, me], s_ls.at[t, d], s_lr.at[t + 1, me], after, sec(d))

    def c_right(t, d):
        return copy(psend.at[t, d], rrecv.at[t, me], s_ps.at[t, d], s_pr.at[t, me], before, sec(d))

    def c_tn(d):
        return copy(tns, tnr.at[me], s_tns.at[d], s_tnr.at[me], j, sec(d))

    def c_tr(d):
        return copy(trs, trr.at[me], s_trs.at[d], s_trr.at[me], before, sec(d))

    def c_gram(d, p):
        return copy(gsend.at[p], grecv.at[me, p], s_gs.at[d, p], s_gr.at[me, p], j, sec(d))

    def c_unit(d):
        return copy(usend, urecv.at[me], s_us.at[d], s_ur.at[me], after, sec(d))

    def got(ref, sem):
        copy(ref, ref, s_us.at[0], sem, after, me).wait_recv()

    barrier = pltpu.get_barrier_semaphore()
    for d in range(parts):
        for where in (after, before) if d == 0 else (after, before, j):
            pl.semaphore_signal(
                barrier, inc=1, device_id={"site": where, "sec": sec(d)}, device_id_type=MESH
            )
    loads[0].wait()
    pl.semaphore_wait(barrier, 3 * parts - 1)
    for d in range(1, parts):
        c_seed(d).start()

    sources = [[src[0, s, off + k] for k in range(owned)] for s in range(phys)]

    def gathered(target):
        total = None
        for s in range(phys):
            hit, at = jnp.int32(0), jnp.int32(0)
            for k in range(owned):
                same = (sources[s][k] == target).astype(jnp.int32)
                hit, at = hit + same, at + same * k
            term = terms[s * owned + at] * hit.astype(F32)
            total = term if total is None else total + term
        return total

    rows = lax.broadcasted_iota(jnp.int32, (width, width), 0)
    cols = lax.broadcasted_iota(jnp.int32, (width, width), 1)
    diagonal = (rows == cols).astype(F32)
    half_diagonal = 0.5 * diagonal

    def traces(blocks):
        total = None
        for block in blocks:
            total = block.astype(F32) if total is None else total + block.astype(F32)
        return jnp.sum((total * diagonal).reshape(width // 8, 8, width), axis=0)

    loads[1].wait()
    for k in range(owned):
        env_r[k] = rseed[0, k]
    loads[2].wait()

    def seed_arrival():
        for k in range(owned):
            hold_l[off + k] = lseed[0, k]
        for d in range(1, parts):
            a = sec(d)
            got(lrecv.at[0, a], s_lr.at[0, a])
            for k in range(owned):
                hold_l[a * owned + k] = lrecv[0, a, k]

    def left_arrival(t):
        for d in range(parts):
            a = sec(d)
            got(lrecv.at[t, a], s_lr.at[t, a])
            for k in range(owned):
                hold_l[a * owned + k] = lrecv[t, a, k]

    def right_arrival(t):
        for d in range(parts):
            a = sec(d)
            got(rrecv.at[t, a], s_pr.at[t, a])
        for k in range(owned):
            total = rrecv[t, 0, k].astype(F32)
            for a in range(1, parts):
                total = total + rrecv[t, a, k].astype(F32)
            env_r[k] = total.astype(BF16)

    def right_compute(t, last):
        for k in range(owned):
            stack = jnp.concatenate([rc[0, s, k] for s in range(phys)], axis=0)
            prod = dot(stack, env_r[k]).astype(BF16)
            for s in range(phys):
                terms[s * owned + k] = dot_nt(prod[s * width : (s + 1) * width], rc[0, s, k])
        for d in range(parts - 1, -1, -1):
            for i in range(owned):
                psend[t, d, i] = gathered(sec(d) * owned + i).astype(BF16)
            if not last:
                c_right(t, d).start()
        if last:
            trs[...] = traces([psend[t, d, i] for d in range(parts) for i in range(owned)])
            for d in range(parts - 1, -1, -1):
                c_tr(d).start()
            for d in range(parts - 1, -1, -1):
                c_right(t, d).start()

    def left_compute(t, last):
        for k in range(owned):
            prods = [
                dot(hold_l[sources[s][k]], lc[0, s, k]).astype(BF16) for s in range(phys)
            ]
            lsend[t, k] = dot(lct[k], jnp.concatenate(prods, axis=0)).astype(BF16)
        if last:
            tns[...] = traces([lsend[t, k] for k in range(owned)])
            for d in range(1, parts):
                c_tn(d).start()
        for d in range(parts - 1, -1, -1):
            c_left(t, d).start()

    right_compute(0, steps == 1)
    loads[3].wait()
    for k in range(owned):
        for s in range(phys):
            lct[k, :, s * width : (s + 1) * width] = lc[0, s, k].T
    seed_arrival()
    left_compute(0, steps == 1)

    def turn(t, carry):
        right_arrival(t - 1)
        right_compute(t, False)
        left_arrival(t)
        left_compute(t, False)
        return carry

    lax.fori_loop(1, steps - 1, turn, 0)
    if steps > 1:
        right_arrival(steps - 2)
        right_compute(steps - 1, True)
        left_arrival(steps - 1)
        left_compute(steps - 1, True)

    def scale_of(total):
        return (sectors * width) / jnp.sum(total, axis=(0, 1), keepdims=True)

    def begin(i, y, z, gram):
        norm = jnp.sqrt(jnp.sum(gram * gram, axis=(0, 1), keepdims=True))
        root = lax.rsqrt(norm)
        delta = (half_diagonal - 0.5 * (gram / norm)).astype(BF16)
        if z is None:
            y = gram / norm
            zs[i] = diagonal + delta.astype(F32)
        else:
            y, z = y * root, z * root
            zs[i] = z + dot(twice_wide(delta), below(split(z)))
        ys[i] = y + dot(beside(split(y)), twice_tall(delta))
        return root

    def deltas(these):
        zh = [split(zs[i]) for i in these]
        yh = [split(ys[i]) for i in these]
        found = [
            (half_diagonal - 0.5 * dot(z[0], y[0])).astype(BF16) for z, y in zip(zh, yh)
        ]
        return zh, yh, found

    def advance(these):
        zh, yh, found = deltas(these)
        for i, z, y, delta in zip(these, zh, yh, found):
            ys[i] = ys[i] + dot(beside(y), twice_tall(delta))
            zs[i] = zs[i] + dot(twice_wide(delta), below(z))

    def loop(count, these):
        def body(n, carry):
            advance(these)
            return carry

        lax.fori_loop(0, count, body, 0)

    bonds = list(range(owned))
    lefts = [owned + k for k in range(owned)]
    rights = [2 * owned + m for m in range(sectors)]

    right_arrival(steps - 1)
    for a in range(parts):
        got(trr.at[a], s_trr.at[a])
    total = trr[0]
    for a in range(1, parts):
        total = total + trr[a]
    scale = scale_of(total)
    for k in range(owned):
        env_r[k] = (env_r[k].astype(F32) * scale).astype(BF16)

    total = tns[...]
    for d in range(1, parts):
        a = sec(d)
        got(tnr.at[a], s_tnr.at[a])
        total = total + tnr[a]
    scale = scale_of(total)
    loads[4].wait()
    now = [cb[0, k] for k in range(owned)]
    for repeat in range(NAPP):
        for k in range(owned):
            half = dot(lsend[steps - 1, k], now[k]).astype(BF16)
            now[k] = (dot(half, env_r[k]) * scale + shift[0] * now[k].astype(F32)).astype(BF16)
    for k in range(owned):
        begin(k, now[k].astype(F32), now[k].astype(F32).T, dot_tn(now[k], now[k]))
    loads[5].wait()
    for k in range(owned):
        for s in range(phys):
            site[k, s * width : (s + 1) * width] = cs[0, s, k]
    loop(EARLY, bonds)

    left_arrival(steps)
    scale = scale_of(traces([hold_l[m] for m in range(sectors)]))
    for repeat in range(NAPP):
        for k in range(owned):
            halves = [
                dot(hold_l[sources[s][k]], site[k, s * width : (s + 1) * width]).astype(BF16)
                for s in range(phys)
            ]
            whole = dot(jnp.concatenate(halves, axis=0), env_r[k]) * scale
            for s in range(phys):
                part = slice(s * width, (s + 1) * width)
                site[k, part] = (whole[part] + onsite[0, s] * site[k, part].astype(F32)).astype(BF16)

    for k in range(owned):
        for s in range(phys):
            block = site[k, s * width : (s + 1) * width]
            terms[s * owned + k] = dot_nt(block, block)
    for p in range(pairs):
        even, odd = gathered(2 * p), gathered(2 * p + 1)
        gsend[p, :width] = jnp.where(rows >= cols, even, odd)
        gsend[p, width:] = jnp.sum((odd * diagonal).reshape(width // 8, 8, width), axis=0)
        for d in range(1, parts):
            c_gram(d, p).start()

    left_root = [
        begin(lefts[k], None, None, dot_tn(site[k], site[k])) for k in range(owned)
    ]
    loop(NSI - 1 - EARLY, bonds + lefts)
    for k in range(owned):
        usend[k] = zs[k].astype(BF16)
    for d in range(parts - 1, -1, -1):
        c_unit(d).start()
    loop(EARLY - 1, lefts)
    zh, yh, found = deltas(lefts)
    for k in range(owned):
        hi, lo = split(zs[k])
        wide = dot(beside(zh[k]), beside((twice_tall(hi), twice_tall(lo))))
        value = wide[:, :width] + wide[:, width:]
        factor = value + dot(twice_wide(found[k]), below(split(value)))
        whole = dot(site[k], (factor * left_root[k]).astype(BF16)).astype(BF16)
        for s in range(phys):
            left_new[s * owned + k][...] = whole[s * width : (s + 1) * width]

    right_root = []
    for p in range(pairs):
        total, edge = gsend[p, :width], gsend[p, width:]
        for d in range(1, parts):
            a = sec(d)
            got(grecv.at[a, p], s_gr.at[a, p])
            total, edge = total + grecv[a, p, :width], edge + grecv[a, p, width:]
        turned = total.T
        line = jnp.sum(edge, axis=0, keepdims=True)
        right_root.append(begin(rights[2 * p], None, None, jnp.where(rows >= cols, total, turned)))
        odd = jnp.where(rows < cols, total, jnp.where(rows == cols, line, turned))
        right_root.append(begin(rights[2 * p + 1], None, None, odd))
    loop(NSI - 2, rights)
    zh, yh, found = deltas(rights)
    for a in range(parts):
        got(urecv.at[a], s_ur.at[a])
    for m in range(sectors):
        unit = urecv[m // owned, m % owned]
        value = dot(twice_wide(unit), below(zh[m]))
        factor = value + dot(beside(split(value)), twice_tall(found[m]))
        fall[m] = (factor * right_root[m]).astype(BF16)
    for k in range(owned):
        for s in range(phys):
            block = site[k, s * width : (s + 1) * width]
            right_new[s * owned + k][...] = dot(fall[sources[s][k]], block).astype(BF16)

    def drain(t, carry):
        for d in range(parts):
            c_left(t, d).wait_send()
            c_right(t, d).wait_send()
        return carry

    lax.fori_loop(0, steps, drain, 0)
    for d in range(parts):
        c_tr(d).wait_send()
        c_unit(d).wait_send()
    for d in range(1, parts):
        c_seed(d).wait_send()
        c_tn(d).wait_send()
        for p in range(pairs):
            c_gram(d, p).wait_send()


def finish(phys, owned, *refs):
    blocks = phys * owned
    left_new, right_new, sems = refs[2 * blocks :]
    copies = []
    for i in range(2 * blocks):
        out = left_new if i < blocks else right_new
        s, k = (i % blocks) // owned, i % owned
        copies.append(pltpu.make_async_copy(refs[i], out.at[0, s, k], sems.at[i]))
        copies[-1].start()
    for c in copies:
        c.wait()


def per_device(lc, rc, cs, cb, lseed, rseed, src, onsite, shift):
    sites, parts = lax.axis_size("site"), lax.axis_size("sec")
    steps = sites // 4
    _, phys, owned, width, _ = lc.shape
    sectors = parts * owned
    pairs = sectors // 2
    block = (width, width)

    def vm(*shape, dtype=BF16):
        return pltpu.VMEM(shape, dtype)

    def dma(*shape):
        return pltpu.SemaphoreType.DMA(shape)

    in_hbm = pl.BlockSpec(memory_space=pltpu.HBM)
    in_vmem = pl.BlockSpec(memory_space=pltpu.VMEM)
    in_smem = pl.BlockSpec(memory_space=pltpu.SMEM)
    shape = jax.ShapeDtypeStruct(cs.shape, BF16)
    blocks = phys * owned
    room = VMEM_BYTES - RESERVED - 2 * cs.size * 2 - SLACK
    done = pl.pallas_call(
        functools.partial(kernel, steps, sites, parts, phys, owned),
        out_shape=[jax.ShapeDtypeStruct(block, BF16)] * (2 * blocks),
        in_specs=[in_hbm] * 6 + [in_smem] * 3,
        out_specs=[in_vmem] * (2 * blocks),
        scratch_shapes=[
            vm(*lc.shape), vm(*rc.shape), vm(*cs.shape), vm(*cb.shape),
            vm(*lseed.shape), vm(*rseed.shape),
            vm(owned, phys * width, width), vm(sectors, *block),
            vm(sectors, *block),
            vm(steps + 1, parts, owned, *block),
            vm(steps, owned, *block),
            vm(steps, parts, owned, *block),
            vm(steps, parts, owned, *block),
            vm(phys * owned, *block, dtype=F32),
            vm(owned, width, phys * width),
            vm(owned, *block),
            vm(2 * owned + sectors, *block, dtype=F32),
            vm(2 * owned + sectors, *block, dtype=F32),
            vm(owned, *block),
            vm(pairs, width + 8, width, dtype=F32),
            vm(parts, pairs, width + 8, width, dtype=F32),
            vm(owned, *block),
            vm(parts, owned, *block),
            vm(8, width, dtype=F32),
            vm(parts, 8, width, dtype=F32),
            vm(8, width, dtype=F32),
            vm(parts, 8, width, dtype=F32),
            dma(6),
            dma(steps + 1, parts), dma(steps + 1, parts),
            dma(steps, parts), dma(steps, parts),
            dma(parts, pairs), dma(parts, pairs),
            dma(parts), dma(parts),
            dma(parts), dma(parts),
            dma(parts), dma(parts),
        ],
        compiler_params=pltpu.CompilerParams(
            collective_id=0, has_side_effects=True, vmem_limit_bytes=room
        ),
    )(lc, rc, cs, cb, lseed, rseed, src, onsite, shift)
    return pl.pallas_call(
        functools.partial(finish, phys, owned),
        out_shape=(shape, shape),
        in_specs=[in_vmem] * (2 * blocks),
        out_specs=(in_hbm, in_hbm),
        scratch_shapes=[dma(2 * blocks)],
        compiler_params=pltpu.CompilerParams(vmem_limit_bytes=8 * 1024 * 1024),
    )(*done)


def solution(mesh):
    tensor = P("site", None, "sec", None, None)
    blocks = P("site", "sec", None, None)
    return jax.shard_map(
        per_device,
        mesh=mesh,
        in_specs=(tensor, tensor, tensor, blocks, blocks, blocks,
                  P("site", None, None), P("site", None), P("site")),
        out_specs=(tensor, tensor),
        check_vma=False,
    )
```

```python
import functools

import jax
import jax.numpy as jnp
from jax import lax
from jax.experimental import pallas as pl
from jax.experimental.pallas import tpu as pltpu
from jax.sharding import PartitionSpec as P

NSI = 10
NAPP = 2
VMEM_BYTES = 67043328
RESERVED = 10240 * 1024
SLACK = 44 * 1024
MESH = pl.DeviceIdType.MESH
F32 = jnp.float32
BF16 = jnp.bfloat16


def dot(a, b):
    return lax.dot_general(a, b, (((1,), (0,)), ((), ())), preferred_element_type=F32)


def dot_nt(a, b):
    return lax.dot_general(a, b, (((1,), (1,)), ((), ())), preferred_element_type=F32)


def dot_tn(a, b):
    return lax.dot_general(a, b, (((0,), (0,)), ((), ())), preferred_element_type=F32)


def split(x):
    hi = x.astype(BF16)
    return hi, (x - hi.astype(F32)).astype(BF16)


def beside(pair):
    return jnp.concatenate(pair, axis=1)


def below(pair):
    return jnp.concatenate(pair, axis=0)


def twice_wide(x):
    return beside((x, x))


def twice_tall(x):
    return below((x, x))


def kernel(
    steps, sites, parts, phys, owned,
    lc_in, rc_in, cs_in, cb_in, lseed_in, rseed_in, src_in, onsite_in, shift_in,
    *refs,
):
    blocks = phys * owned
    left_new, right_new = refs[:blocks], refs[blocks : 2 * blocks]
    (
    lc, rc, cs, cb, lseed, rseed, src, onsite, shift, site, fall,
    hold_l, lrecv, lsend, rrecv, psend, terms, lct, bond, ys, zs, env_r,
    gsend, grecv, usend, urecv, tns, tnr, trs, trr,
    s_in, s_ls, s_lr, s_ps, s_pr, s_gs, s_gr, s_us, s_ur, s_tns, s_tnr, s_trs, s_trr,
    ) = refs[2 * blocks :]
    j = lax.axis_index("site")
    me = lax.axis_index("sec")
    after, before = lax.rem(j + 1, sites), lax.rem(j + sites - 1, sites)
    off = me * owned
    width = lc.shape[-1]
    sectors = parts * owned
    pairs = sectors // 2

    def load(i, a, b):
        return pltpu.make_async_copy(a, b, s_in.at[i])

    loads = [
        load(0, lseed_in, lseed), load(1, rseed_in, rseed), load(2, rc_in, rc),
        load(3, lc_in, lc), load(4, cb_in, cb), load(5, cs_in, cs),
        load(6, src_in, src), load(7, onsite_in, onsite), load(8, shift_in, shift),
    ]
    for c in loads:
        c.start()

    def sec(d):
        return lax.rem(me + d, parts)

    def copy(a, b, ss, rs, to_site, to_sec):
        return pltpu.make_async_remote_copy(
            src_ref=a, dst_ref=b, send_sem=ss, recv_sem=rs,
            device_id={"site": to_site, "sec": to_sec}, device_id_type=MESH,
        )

    def c_seed(d):
        return copy(lseed.at[0], lrecv.at[0, me], s_ls.at[steps, d, 0], s_lr.at[0, me, 0], j, sec(d))

    def c_left(t, d, k):
        return copy(
            lsend.at[t, k], lrecv.at[t + 1, me, k], s_ls.at[t, d, k], s_lr.at[t + 1, me, k], after, sec(d)
        )

    def c_right(t, d):
        return copy(psend.at[t, d], rrecv.at[t, me], s_ps.at[t, d], s_pr.at[t, me], before, sec(d))

    def c_tn(d):
        return copy(tns, tnr.at[me], s_tns.at[d], s_tnr.at[me], j, sec(d))

    def c_tr(d):
        return copy(trs, trr.at[me], s_trs.at[d], s_trr.at[me], before, sec(d))

    def c_gram(d, p):
        return copy(gsend.at[p], grecv.at[me, p], s_gs.at[d, p], s_gr.at[me, p], j, sec(d))

    def c_unit(d):
        return copy(usend, urecv.at[me], s_us.at[d], s_ur.at[me], after, sec(d))

    def got(ref, sem):
        copy(ref, ref, s_us.at[0], sem, after, me).wait_recv()

    def c_out(side, s, k):
        a, b = (right_new, right_out) if side else (left_new, left_out)
        return pltpu.make_async_copy(a.at[0, s, k], b.at[0, s, k], s_out.at[side, s, k])

    barrier = pltpu.get_barrier_semaphore()
    for d in range(parts):
        for where in (after, before) if d == 0 else (after, before, j):
            pl.semaphore_signal(
                barrier, inc=1, device_id={"site": where, "sec": sec(d)}, device_id_type=MESH
            )
    loads[0].wait()
    pl.semaphore_wait(barrier, 3 * parts - 1)
    for d in range(1, parts):
        c_seed(d).start()

    for c in loads[6:]:
        c.wait()
    sources = [[src[0, s, off + k] for k in range(owned)] for s in range(phys)]

    def gathered(target):
        total = None
        for s in range(phys):
            hit, at = jnp.int32(0), jnp.int32(0)
            for k in range(owned):
                same = (sources[s][k] == target).astype(jnp.int32)
                hit, at = hit + same, at + same * k
            term = terms[s * owned + at] * hit.astype(F32)
            total = term if total is None else total + term
        return total

    rows = lax.broadcasted_iota(jnp.int32, (width, width), 0)
    cols = lax.broadcasted_iota(jnp.int32, (width, width), 1)
    diagonal = (rows == cols).astype(F32)
    half_diagonal = 0.5 * diagonal

    def traces(blocks):
        total = None
        for block in blocks:
            total = block.astype(F32) if total is None else total + block.astype(F32)
        return jnp.sum((total * diagonal).reshape(width // 8, 8, width), axis=0)

    loads[1].wait()
    for k in range(owned):
        env_r[k] = rseed[0, k]
    loads[2].wait()

    def seed_arrival():
        for k in range(owned):
            hold_l[off + k] = lseed[0, k]
        for d in range(1, parts):
            a = sec(d)
            got(lrecv.at[0, a], s_lr.at[0, a, 0])
            for k in range(owned):
                hold_l[a * owned + k] = lrecv[0, a, k]

    def left_arrival(t):
        for d in range(parts):
            a = sec(d)
            for k in range(owned):
                got(lrecv.at[t, a, k], s_lr.at[t, a, k])
                hold_l[a * owned + k] = lrecv[t, a, k]

    def right_arrival(t):
        for d in range(parts):
            a = sec(d)
            got(rrecv.at[t, a], s_pr.at[t, a])
        for k in range(owned):
            total = rrecv[t, 0, k].astype(F32)
            for a in range(1, parts):
                total = total + rrecv[t, a, k].astype(F32)
            env_r[k] = total.astype(BF16)

    def right_compute(t, last):
        for k in range(owned):
            stack = jnp.concatenate([rc[0, s, k] for s in range(phys)], axis=0)
            prod = dot(stack, env_r[k]).astype(BF16)
            for s in range(phys):
                terms[s * owned + k] = dot_nt(prod[s * width : (s + 1) * width], rc[0, s, k])
        for d in range(parts - 1, -1, -1):
            for i in range(owned):
                psend[t, d, i] = gathered(sec(d) * owned + i).astype(BF16)
            if not last:
                c_right(t, d).start()
        if last:
            trs[...] = traces([psend[t, d, i] for d in range(parts) for i in range(owned)])
            for d in range(parts - 1, -1, -1):
                c_tr(d).start()
            for d in range(parts - 1, -1, -1):
                c_right(t, d).start()

    def left_compute(t, last):
        prods = [
            [dot(hold_l[sources[s][k]], lc[0, s, k]).astype(BF16) for s in range(phys)]
            for k in range(owned)
        ]
        for k in range(owned):
            lsend[t, k] = dot(lct[k], below(prods[k])).astype(BF16)
            if last and k == owned - 1:
                tns[...] = traces([lsend[t, i] for i in range(owned)])
                for d in range(1, parts):
                    c_tn(d).start()
            for d in range(parts - 1, -1, -1):
                c_left(t, d, k).start()

    right_compute(0, steps == 1)
    loads[3].wait()
    for k in range(owned):
        for s in range(phys):
            lct[k, :, s * width : (s + 1) * width] = lc[0, s, k].T
    seed_arrival()
    left_compute(0, steps == 1)

    def turn(t, carry):
        right_arrival(t - 1)
        right_compute(t, False)
        left_arrival(t)
        left_compute(t, False)
        return carry

    lax.fori_loop(1, steps - 1, turn, 0)
    if steps > 1:
        right_arrival(steps - 2)
        right_compute(steps - 1, True)
        left_arrival(steps - 1)
        left_compute(steps - 1, True)

    def scale_of(total):
        return (sectors * width) / jnp.sum(total, axis=(0, 1), keepdims=True)

    def begin(i, gram, block=None):
        norm = jnp.sqrt(jnp.sum(gram * gram, axis=(0, 1), keepdims=True))
        back, root = 1.0 / norm, 1.0 / jnp.sqrt(norm)
        hi, lo = split(gram)
        if block is None:
            square = dot(beside((hi, lo)), twice_tall(hi))
            first = gram * back
            ys[i] = 1.5 * first - 0.5 * ((square * back) * back)
            zs[i] = 1.5 * diagonal - 0.5 * first
        else:
            turned = block.T
            ys[i] = (1.5 * block.astype(F32) - 0.5 * (dot(block, hi) * back)) * root
            zs[i] = (1.5 * turned.astype(F32) - 0.5 * (dot(hi, turned) * back)) * root
        return root

    def deltas(these, swap=False):
        zh = [split(zs[i]) for i in these]
        yh = [split(ys[i]) for i in these]
        found = [
            (half_diagonal - 0.5 * (dot(y[0], z[0]) if swap else dot(z[0], y[0]))).astype(BF16)
            for z, y in zip(zh, yh)
        ]
        return zh, yh, found

    def advance(these):
        zh, yh, found = deltas(these)
        for i, z, y, delta in zip(these, zh, yh, found):
            ys[i] = ys[i] + dot(beside(y), twice_tall(delta))
            zs[i] = zs[i] + dot(twice_wide(delta), below(z))

    def loop(count, these):
        def body(n, carry):
            advance(these)
            return carry

        lax.fori_loop(0, count, body, 0)

    bonds = list(range(owned))
    lefts = [owned + k for k in range(owned)]
    rights = [2 * owned + m for m in range(sectors)]

    right_arrival(steps - 1)
    for a in range(parts):
        got(trr.at[a], s_trr.at[a])
    total = trr[0]
    for a in range(1, parts):
        total = total + trr[a]
    scale = scale_of(total)
    for k in range(owned):
        env_r[k] = (env_r[k].astype(F32) * scale).astype(BF16)

    total = tns[...]
    for d in range(1, parts):
        a = sec(d)
        got(tnr.at[a], s_tnr.at[a])
        total = total + tnr[a]
    scale = scale_of(total)
    loads[4].wait()
    now = [cb[0, k] for k in range(owned)]
    for repeat in range(NAPP):
        for k in range(owned):
            half = dot(lsend[steps - 1, k], now[k]).astype(BF16)
            now[k] = (dot(half, env_r[k]) * scale + shift[0] * now[k].astype(F32)).astype(BF16)
    for k in range(owned):
        begin(bonds[k], dot_tn(now[k], now[k]), now[k])
    loads[5].wait()
    for k in range(owned):
        for s in range(phys):
            site[k, s * width : (s + 1) * width] = cs[0, s, k]

    left_arrival(steps)
    scale = scale_of(traces([hold_l[m] for m in range(sectors)]))
    for repeat in range(NAPP):
        for k in range(owned):
            halves = [
                dot(hold_l[sources[s][k]], site[k, s * width : (s + 1) * width]).astype(BF16)
                for s in range(phys)
            ]
            whole = dot(jnp.concatenate(halves, axis=0), env_r[k]) * scale
            for s in range(phys):
                part = slice(s * width, (s + 1) * width)
                site[k, part] = (whole[part] + onsite[0, s] * site[k, part].astype(F32)).astype(BF16)

    for k in range(owned):
        for s in range(phys):
            block = site[k, s * width : (s + 1) * width]
            terms[s * owned + k] = dot_nt(block, block)
    for p in range(pairs):
        even, odd = gathered(2 * p), gathered(2 * p + 1)
        gsend[p, :width] = jnp.where(rows >= cols, even, odd)
        gsend[p, width:] = jnp.sum((odd * diagonal).reshape(width // 8, 8, width), axis=0)
        for d in range(1, parts):
            c_gram(d, p).start()

    left_root = [
        begin(lefts[k], dot_tn(site[k], site[k])) for k in range(owned)
    ]
    advance(bonds)
    loop(NSI - 2, bonds + lefts)
    for k in range(owned):
        usend[k] = zs[k].astype(BF16)
    for d in range(parts - 1, -1, -1):
        c_unit(d).start()
    packed = []
    for p in range(pairs):
        total, edge = gsend[p, :width], gsend[p, width:]
        for d in range(1, parts):
            a = sec(d)
            got(grecv.at[a, p], s_gr.at[a, p])
            total, edge = total + grecv[a, p, :width], edge + grecv[a, p, width:]
        packed.append((total, jnp.sum(edge, axis=0, keepdims=True)))
    right_root = []
    for p, (total, line) in enumerate(packed):
        turned = total.T
        right_root.append(begin(rights[2 * p], jnp.where(rows >= cols, total, turned)))
        odd = jnp.where(rows < cols, total, jnp.where(rows == cols, line, turned))
        right_root.append(begin(rights[2 * p + 1], odd))
    zh, yh, found = deltas(lefts)
    for k in range(owned):
        hi, lo = split(zs[k])
        wide = dot(beside(zh[k]), beside((twice_tall(hi), twice_tall(lo))))
        value = wide[:, :width] + wide[:, width:]
        factor = value + dot(twice_wide(found[k]), below(split(value)))
        whole = dot(site[k], (factor * left_root[k]).astype(BF16)).astype(BF16)
        for s in range(phys):
            left_new[s * owned + k][...] = whole[s * width : (s + 1) * width]

    loop(NSI - 2, rights)
    zh, yh, found = deltas(rights, swap=True)
    for a in range(parts):
        got(urecv.at[a], s_ur.at[a])
    for m in range(sectors):
        unit = urecv[m // owned, m % owned]
        value = dot(twice_wide(unit), below(zh[m]))
        factor = value + dot(beside(split(value)), twice_tall(found[m]))
        fall[m] = (factor * right_root[m]).astype(BF16)
    for k in range(owned):
        for s in range(phys):
            block = site[k, s * width : (s + 1) * width]
            right_new[s * owned + k][...] = dot(fall[sources[s][k]], block).astype(BF16)

    def drain(t, carry):
        for d in range(parts):
            for k in range(owned):
                c_left(t, d, k).wait_send()
            c_right(t, d).wait_send()
        return carry

    lax.fori_loop(0, steps, drain, 0)
    for d in range(parts):
        c_tr(d).wait_send()
        c_unit(d).wait_send()
    for d in range(1, parts):
        c_seed(d).wait_send()
        c_tn(d).wait_send()
        for p in range(pairs):
            c_gram(d, p).wait_send()


def finish(phys, owned, *refs):
    blocks = phys * owned
    left_new, right_new, sems = refs[2 * blocks :]
    copies = []
    for i in range(2 * blocks):
        out = left_new if i < blocks else right_new
        s, k = (i % blocks) // owned, i % owned
        copies.append(pltpu.make_async_copy(refs[i], out.at[0, s, k], sems.at[i]))
        copies[-1].start()
    for c in copies:
        c.wait()


def per_device(lc, rc, cs, cb, lseed, rseed, src, onsite, shift):
    sites, parts = lax.axis_size("site"), lax.axis_size("sec")
    steps = sites // 4
    _, phys, owned, width, _ = lc.shape
    sectors = parts * owned
    pairs = sectors // 2
    block = (width, width)

    def vm(*shape, dtype=BF16):
        return pltpu.VMEM(shape, dtype)

    def dma(*shape):
        return pltpu.SemaphoreType.DMA(shape)

    in_hbm = pl.BlockSpec(memory_space=pltpu.HBM)
    in_vmem = pl.BlockSpec(memory_space=pltpu.VMEM)
    shape = jax.ShapeDtypeStruct(cs.shape, BF16)
    blocks = phys * owned
    room = VMEM_BYTES - RESERVED - 2 * cs.size * 2 - SLACK
    done = pl.pallas_call(
        functools.partial(kernel, steps, sites, parts, phys, owned),
        out_shape=[jax.ShapeDtypeStruct(block, BF16)] * (2 * blocks),
        in_specs=[in_hbm] * 9,
        out_specs=[in_vmem] * (2 * blocks),
        scratch_shapes=[
            vm(*lc.shape), vm(*rc.shape), vm(*cs.shape), vm(*cb.shape),
            vm(*lseed.shape), vm(*rseed.shape),
            pltpu.SMEM(src.shape, src.dtype), pltpu.SMEM(onsite.shape, F32), pltpu.SMEM(shift.shape, F32),
            vm(owned, phys * width, width), vm(sectors, *block),
            vm(sectors, *block),
            vm(steps + 1, parts, owned, *block),
            vm(steps, owned, *block),
            vm(steps, parts, owned, *block),
            vm(steps, parts, owned, *block),
            vm(phys * owned, *block, dtype=F32),
            vm(owned, width, phys * width),
            vm(owned, *block),
            vm(2 * owned + sectors, *block, dtype=F32),
            vm(2 * owned + sectors, *block, dtype=F32),
            vm(owned, *block),
            vm(pairs, width + 8, width, dtype=F32),
            vm(parts, pairs, width + 8, width, dtype=F32),
            vm(owned, *block),
            vm(parts, owned, *block),
            vm(8, width, dtype=F32),
            vm(parts, 8, width, dtype=F32),
            vm(8, width, dtype=F32),
            vm(parts, 8, width, dtype=F32),
            dma(9),
            dma(steps + 1, parts, owned), dma(steps + 1, parts, owned),
            dma(steps, parts), dma(steps, parts),
            dma(parts, pairs), dma(parts, pairs),
            dma(parts), dma(parts),
            dma(parts), dma(parts),
            dma(parts), dma(parts),
        ],
        compiler_params=pltpu.CompilerParams(
            collective_id=0, has_side_effects=True, vmem_limit_bytes=room
        ),
    )(lc, rc, cs, cb, lseed, rseed, src, onsite, shift)
    return pl.pallas_call(
        functools.partial(finish, phys, owned),
        out_shape=(shape, shape),
        in_specs=[in_vmem] * (2 * blocks),
        out_specs=(in_hbm, in_hbm),
        scratch_shapes=[dma(2 * blocks)],
        compiler_params=pltpu.CompilerParams(vmem_limit_bytes=8 * 1024 * 1024),
    )(*done)


def solution(mesh):
    tensor = P("site", None, "sec", None, None)
    blocks = P("site", "sec", None, None)
    return jax.shard_map(
        per_device,
        mesh=mesh,
        in_specs=(tensor, tensor, tensor, blocks, blocks, blocks,
                  P("site", None, None), P("site", None), P("site")),
        out_specs=(tensor, tensor),
        check_vma=False,
    )
```

```python
import functools

import jax
import jax.numpy as jnp
from jax import lax
from jax.experimental import pallas as pl
from jax.experimental.pallas import tpu as pltpu
from jax.sharding import PartitionSpec as P

NSI = 10
NAPP = 2
UNROLL = 4
VMEM_BYTES = 67043328
RESERVED = 10240 * 1024
SLACK = 44 * 1024
MESH = pl.DeviceIdType.MESH
F32 = jnp.float32
BF16 = jnp.bfloat16


def dot(a, b):
    return lax.dot_general(a, b, (((1,), (0,)), ((), ())), preferred_element_type=F32)


def dot_nt(a, b):
    return lax.dot_general(a, b, (((1,), (1,)), ((), ())), preferred_element_type=F32)


def dot_tn(a, b):
    return lax.dot_general(a, b, (((0,), (0,)), ((), ())), preferred_element_type=F32)


def split(x):
    hi = x.astype(BF16)
    return hi, (x - hi.astype(F32)).astype(BF16)


def beside(pair):
    return jnp.concatenate(pair, axis=1)


def below(pair):
    return jnp.concatenate(pair, axis=0)


def twice_wide(x):
    return beside((x, x))


def twice_tall(x):
    return below((x, x))


def kernel(
    steps, sites, parts, phys, owned,
    lc_in, rc_in, cs_in, cb_in, lseed_in, rseed_in, src_in, onsite_in, shift_in,
    *refs,
):
    blocks = phys * owned
    left_new, right_new = refs[:blocks], refs[blocks : 2 * blocks]
    (
    lc, rc, cs, cb, lseed, rseed, src, onsite, shift, site, fall,
    hold_l, lrecv, lsend, rrecv, psend, terms, lct, bond, ys, zs, env_r,
    gsend, grecv, usend, urecv, tns, tnr, trs, trr,
    s_in, s_ls, s_lr, s_ps, s_pr, s_gs, s_gr, s_us, s_ur, s_tns, s_tnr, s_trs, s_trr,
    ) = refs[2 * blocks :]
    j = lax.axis_index("site")
    me = lax.axis_index("sec")
    after, before = lax.rem(j + 1, sites), lax.rem(j + sites - 1, sites)
    off = me * owned
    width = lc.shape[-1]
    sectors = parts * owned
    pairs = sectors // 2

    def load(i, a, b):
        return pltpu.make_async_copy(a, b, s_in.at[i])

    loads = [
        load(0, lseed_in, lseed), load(1, rseed_in, rseed), load(2, rc_in, rc),
        load(3, lc_in, lc), load(4, cb_in, cb), load(5, cs_in, cs),
        load(6, src_in, src), load(7, onsite_in, onsite), load(8, shift_in, shift),
    ]
    for c in loads:
        c.start()

    def sec(d):
        return lax.rem(me + d, parts)

    def copy(a, b, ss, rs, to_site, to_sec):
        return pltpu.make_async_remote_copy(
            src_ref=a, dst_ref=b, send_sem=ss, recv_sem=rs,
            device_id={"site": to_site, "sec": to_sec}, device_id_type=MESH,
        )

    def c_seed(d):
        return copy(lseed.at[0], lrecv.at[0, me], s_ls.at[steps, d, 0], s_lr.at[0, me, 0], j, sec(d))

    def c_left(t, d, k):
        return copy(
            lsend.at[t, k], lrecv.at[t + 1, me, k], s_ls.at[t, d, k], s_lr.at[t + 1, me, k], after, sec(d)
        )

    def c_right(t, d):
        return copy(psend.at[t, d], rrecv.at[t, me], s_ps.at[t, d], s_pr.at[t, me], before, sec(d))

    def c_tn(d):
        return copy(tns, tnr.at[me], s_tns.at[d], s_tnr.at[me], j, sec(d))

    def c_tr(d):
        return copy(trs, trr.at[me], s_trs.at[d], s_trr.at[me], before, sec(d))

    def c_gram(d, p):
        return copy(gsend.at[p], grecv.at[me, p], s_gs.at[d, p], s_gr.at[me, p], j, sec(d))

    def c_unit(d):
        return copy(usend, urecv.at[me], s_us.at[d], s_ur.at[me], after, sec(d))

    def got(ref, sem):
        copy(ref, ref, s_us.at[0], sem, after, me).wait_recv()

    def c_out(side, s, k):
        a, b = (right_new, right_out) if side else (left_new, left_out)
        return pltpu.make_async_copy(a.at[0, s, k], b.at[0, s, k], s_out.at[side, s, k])

    barrier = pltpu.get_barrier_semaphore()
    for d in range(parts):
        for where in (after, before) if d == 0 else (after, before, j):
            pl.semaphore_signal(
                barrier, inc=1, device_id={"site": where, "sec": sec(d)}, device_id_type=MESH
            )
    loads[0].wait()
    pl.semaphore_wait(barrier, 3 * parts - 1)
    for d in range(1, parts):
        c_seed(d).start()

    for c in loads[6:]:
        c.wait()
    sources = [[src[0, s, off + k] for k in range(owned)] for s in range(phys)]

    def gathered(target):
        total = None
        for s in range(phys):
            hit, at = jnp.int32(0), jnp.int32(0)
            for k in range(owned):
                same = (sources[s][k] == target).astype(jnp.int32)
                hit, at = hit + same, at + same * k
            term = terms[s * owned + at] * hit.astype(F32)
            total = term if total is None else total + term
        return total

    rows = lax.broadcasted_iota(jnp.int32, (width, width), 0)
    cols = lax.broadcasted_iota(jnp.int32, (width, width), 1)
    diagonal = (rows == cols).astype(F32)
    half_diagonal = 0.5 * diagonal

    def traces(blocks):
        total = None
        for block in blocks:
            total = block.astype(F32) if total is None else total + block.astype(F32)
        return jnp.sum((total * diagonal).reshape(width // 8, 8, width), axis=0)

    loads[1].wait()
    for k in range(owned):
        env_r[k] = rseed[0, k]
    loads[2].wait()

    def seed_arrival():
        for k in range(owned):
            hold_l[off + k] = lseed[0, k]
        for d in range(1, parts):
            a = sec(d)
            got(lrecv.at[0, a], s_lr.at[0, a, 0])
            for k in range(owned):
                hold_l[a * owned + k] = lrecv[0, a, k]

    def left_arrival(t):
        for d in range(parts):
            a = sec(d)
            for k in range(owned):
                got(lrecv.at[t, a, k], s_lr.at[t, a, k])
                hold_l[a * owned + k] = lrecv[t, a, k]

    def right_arrival(t):
        for d in range(parts):
            a = sec(d)
            got(rrecv.at[t, a], s_pr.at[t, a])
        for k in range(owned):
            total = rrecv[t, 0, k].astype(F32)
            for a in range(1, parts):
                total = total + rrecv[t, a, k].astype(F32)
            env_r[k] = total.astype(BF16)

    def right_compute(t, last):
        for k in range(owned):
            stack = jnp.concatenate([rc[0, s, k] for s in range(phys)], axis=0)
            prod = dot(stack, env_r[k]).astype(BF16)
            for s in range(phys):
                terms[s * owned + k] = dot_nt(prod[s * width : (s + 1) * width], rc[0, s, k])
        for d in range(parts - 1, -1, -1):
            for i in range(owned):
                psend[t, d, i] = gathered(sec(d) * owned + i).astype(BF16)
            if not last:
                c_right(t, d).start()
        if last:
            trs[...] = traces([psend[t, d, i] for d in range(parts) for i in range(owned)])
            for d in range(parts - 1, -1, -1):
                c_tr(d).start()
            for d in range(parts - 1, -1, -1):
                c_right(t, d).start()

    def left_compute(t, last):
        prods = [
            [dot(hold_l[sources[s][k]], lc[0, s, k]).astype(BF16) for s in range(phys)]
            for k in range(owned)
        ]
        for k in range(owned):
            lsend[t, k] = dot(lct[k], below(prods[k])).astype(BF16)
            if last and k == owned - 1:
                tns[...] = traces([lsend[t, i] for i in range(owned)])
                for d in range(1, parts):
                    c_tn(d).start()
            for d in range(parts - 1, -1, -1):
                c_left(t, d, k).start()

    right_compute(0, steps == 1)
    loads[3].wait()
    for k in range(owned):
        for s in range(phys):
            lct[k, :, s * width : (s + 1) * width] = lc[0, s, k].T
    seed_arrival()
    left_compute(0, steps == 1)

    def turn(t, carry):
        right_arrival(t - 1)
        right_compute(t, False)
        left_arrival(t)
        left_compute(t, False)
        return carry

    lax.fori_loop(1, steps - 1, turn, 0)
    if steps > 1:
        right_arrival(steps - 2)
        right_compute(steps - 1, True)
        left_arrival(steps - 1)
        left_compute(steps - 1, True)

    def scale_of(total):
        return (sectors * width) / jnp.sum(total, axis=(0, 1), keepdims=True)

    def begin(i, gram, block=None):
        norm = jnp.sqrt(jnp.sum(gram * gram, axis=(0, 1), keepdims=True))
        back, root = 1.0 / norm, 1.0 / jnp.sqrt(norm)
        hi, lo = split(gram)
        if block is None:
            square = dot(beside((hi, lo)), twice_tall(hi))
            first = gram * back
            ys[i] = 1.5 * first - 0.5 * ((square * back) * back)
            zs[i] = 1.5 * diagonal - 0.5 * first
        else:
            turned = block.T
            ys[i] = (1.5 * block.astype(F32) - 0.5 * (dot(block, hi) * back)) * root
            zs[i] = (1.5 * turned.astype(F32) - 0.5 * (dot(hi, turned) * back)) * root
        return root

    def deltas(these, swap=False):
        zh = [split(zs[i]) for i in these]
        yh = [split(ys[i]) for i in these]
        found = [
            (half_diagonal - 0.5 * (dot(y[0], z[0]) if swap else dot(z[0], y[0]))).astype(BF16)
            for z, y in zip(zh, yh)
        ]
        return zh, yh, found

    def advance(these):
        zh, yh, found = deltas(these)
        for i, z, y, delta in zip(these, zh, yh, found):
            ys[i] = ys[i] + dot(beside(y), twice_tall(delta))
            zs[i] = zs[i] + dot(twice_wide(delta), below(z))

    def loop(count, these):
        def body(n, carry):
            for again in range(UNROLL):
                advance(these)
            return carry

        lax.fori_loop(0, count // UNROLL, body, 0)
        for again in range(count % UNROLL):
            advance(these)

    bonds = list(range(owned))
    lefts = [owned + k for k in range(owned)]
    rights = [2 * owned + m for m in range(sectors)]

    right_arrival(steps - 1)
    for a in range(parts):
        got(trr.at[a], s_trr.at[a])
    total = trr[0]
    for a in range(1, parts):
        total = total + trr[a]
    scale = scale_of(total)
    for k in range(owned):
        env_r[k] = (env_r[k].astype(F32) * scale).astype(BF16)

    loads[4].wait()
    now = [cb[0, k] for k in range(owned)]

    def bond_product(k):
        return dot(dot(lsend[steps - 1, k], now[k]).astype(BF16), env_r[k])

    product = [bond_product(k) for k in range(owned)]
    total = tns[...]
    for d in range(1, parts):
        a = sec(d)
        got(tnr.at[a], s_tnr.at[a])
        total = total + tnr[a]
    bond_scale = scale_of(total)
    loads[5].wait()
    for k in range(owned):
        for s in range(phys):
            site[k, s * width : (s + 1) * width] = cs[0, s, k]

    left_arrival(steps)
    scale = scale_of(traces([hold_l[m] for m in range(sectors)]))
    for repeat in range(NAPP):
        for k in range(owned):
            halves = [
                dot(hold_l[sources[s][k]], site[k, s * width : (s + 1) * width]).astype(BF16)
                for s in range(phys)
            ]
            whole = dot(jnp.concatenate(halves, axis=0), env_r[k]) * scale
            for s in range(phys):
                part = slice(s * width, (s + 1) * width)
                site[k, part] = (whole[part] + onsite[0, s] * site[k, part].astype(F32)).astype(BF16)

    for k in range(owned):
        for s in range(phys):
            block = site[k, s * width : (s + 1) * width]
            terms[s * owned + k] = dot_nt(block, block)
    for p in range(pairs):
        even, odd = gathered(2 * p), gathered(2 * p + 1)
        gsend[p, :width] = jnp.where(rows >= cols, even, odd)
        gsend[p, width:] = jnp.sum((odd * diagonal).reshape(width // 8, 8, width), axis=0)
        for d in range(1, parts):
            c_gram(d, p).start()

    for repeat in range(NAPP):
        if repeat > 0:
            product = [bond_product(k) for k in range(owned)]
        for k in range(owned):
            now[k] = (product[k] * bond_scale + shift[0] * now[k].astype(F32)).astype(BF16)
    for k in range(owned):
        begin(bonds[k], dot_tn(now[k], now[k]), now[k])
    left_root = [
        begin(lefts[k], dot_tn(site[k], site[k])) for k in range(owned)
    ]
    loop(NSI - 2, bonds + lefts)
    advance(bonds)
    for k in range(owned):
        usend[k] = zs[k].astype(BF16)
    for d in range(parts - 1, -1, -1):
        c_unit(d).start()
    zh, yh, found = deltas(lefts)
    for k in range(owned):
        hi, lo = split(zs[k])
        wide = dot(beside(zh[k]), beside((twice_tall(hi), twice_tall(lo))))
        value = wide[:, :width] + wide[:, width:]
        factor = value + dot(twice_wide(found[k]), below(split(value)))
        whole = dot(site[k], (factor * left_root[k]).astype(BF16)).astype(BF16)
        for s in range(phys):
            left_new[s * owned + k][...] = whole[s * width : (s + 1) * width]

    packed = []
    for p in range(pairs):
        total, edge = gsend[p, :width], gsend[p, width:]
        for d in range(1, parts):
            a = sec(d)
            got(grecv.at[a, p], s_gr.at[a, p])
            total, edge = total + grecv[a, p, :width], edge + grecv[a, p, width:]
        packed.append((total, jnp.sum(edge, axis=0, keepdims=True)))
    right_root = []
    for p, (total, line) in enumerate(packed):
        turned = total.T
        right_root.append(begin(rights[2 * p], jnp.where(rows >= cols, total, turned)))
        odd = jnp.where(rows < cols, total, jnp.where(rows == cols, line, turned))
        right_root.append(begin(rights[2 * p + 1], odd))
    loop(NSI - 2, rights)
    for a in range(parts):
        got(urecv.at[a], s_ur.at[a])
    zh, yh, found = deltas(rights, swap=True)
    values = [
        dot(twice_wide(urecv[m // owned, m % owned]), below(zh[m])) for m in range(sectors)
    ]
    for m in range(sectors):
        factor = values[m] + dot(beside(split(values[m])), twice_tall(found[m]))
        fall[m] = (factor * right_root[m]).astype(BF16)
    for k in range(owned):
        for s in range(phys):
            block = site[k, s * width : (s + 1) * width]
            right_new[s * owned + k][...] = dot(fall[sources[s][k]], block).astype(BF16)

    def drain(t, carry):
        for d in range(parts):
            for k in range(owned):
                c_left(t, d, k).wait_send()
            c_right(t, d).wait_send()
        return carry

    lax.fori_loop(0, steps, drain, 0)
    for d in range(parts):
        c_tr(d).wait_send()
        c_unit(d).wait_send()
    for d in range(1, parts):
        c_seed(d).wait_send()
        c_tn(d).wait_send()
        for p in range(pairs):
            c_gram(d, p).wait_send()


def finish(phys, owned, *refs):
    blocks = phys * owned
    left_new, right_new, sems = refs[2 * blocks :]
    copies = []
    for i in range(2 * blocks):
        out = left_new if i < blocks else right_new
        s, k = (i % blocks) // owned, i % owned
        copies.append(pltpu.make_async_copy(refs[i], out.at[0, s, k], sems.at[i]))
        copies[-1].start()
    for c in copies:
        c.wait()


def per_device(lc, rc, cs, cb, lseed, rseed, src, onsite, shift):
    sites, parts = lax.axis_size("site"), lax.axis_size("sec")
    steps = sites // 4
    _, phys, owned, width, _ = lc.shape
    sectors = parts * owned
    pairs = sectors // 2
    block = (width, width)

    def vm(*shape, dtype=BF16):
        return pltpu.VMEM(shape, dtype)

    def dma(*shape):
        return pltpu.SemaphoreType.DMA(shape)

    in_hbm = pl.BlockSpec(memory_space=pltpu.HBM)
    in_vmem = pl.BlockSpec(memory_space=pltpu.VMEM)
    shape = jax.ShapeDtypeStruct(cs.shape, BF16)
    blocks = phys * owned
    room = VMEM_BYTES - RESERVED - 2 * cs.size * 2 - SLACK
    done = pl.pallas_call(
        functools.partial(kernel, steps, sites, parts, phys, owned),
        out_shape=[jax.ShapeDtypeStruct(block, BF16)] * (2 * blocks),
        in_specs=[in_hbm] * 9,
        out_specs=[in_vmem] * (2 * blocks),
        scratch_shapes=[
            vm(*lc.shape), vm(*rc.shape), vm(*cs.shape), vm(*cb.shape),
            vm(*lseed.shape), vm(*rseed.shape),
            pltpu.SMEM(src.shape, src.dtype), pltpu.SMEM(onsite.shape, F32), pltpu.SMEM(shift.shape, F32),
            vm(owned, phys * width, width), vm(sectors, *block),
            vm(sectors, *block),
            vm(steps + 1, parts, owned, *block),
            vm(steps, owned, *block),
            vm(steps, parts, owned, *block),
            vm(steps, parts, owned, *block),
            vm(phys * owned, *block, dtype=F32),
            vm(owned, width, phys * width),
            vm(owned, *block),
            vm(2 * owned + sectors, *block, dtype=F32),
            vm(2 * owned + sectors, *block, dtype=F32),
            vm(owned, *block),
            vm(pairs, width + 8, width, dtype=F32),
            vm(parts, pairs, width + 8, width, dtype=F32),
            vm(owned, *block),
            vm(parts, owned, *block),
            vm(8, width, dtype=F32),
            vm(parts, 8, width, dtype=F32),
            vm(8, width, dtype=F32),
            vm(parts, 8, width, dtype=F32),
            dma(9),
            dma(steps + 1, parts, owned), dma(steps + 1, parts, owned),
            dma(steps, parts), dma(steps, parts),
            dma(parts, pairs), dma(parts, pairs),
            dma(parts), dma(parts),
            dma(parts), dma(parts),
            dma(parts), dma(parts),
        ],
        compiler_params=pltpu.CompilerParams(
            collective_id=0, has_side_effects=True, vmem_limit_bytes=room
        ),
    )(lc, rc, cs, cb, lseed, rseed, src, onsite, shift)
    return pl.pallas_call(
        functools.partial(finish, phys, owned),
        out_shape=(shape, shape),
        in_specs=[in_vmem] * (2 * blocks),
        out_specs=(in_hbm, in_hbm),
        scratch_shapes=[dma(2 * blocks)],
        compiler_params=pltpu.CompilerParams(vmem_limit_bytes=8 * 1024 * 1024),
    )(*done)


def solution(mesh):
    tensor = P("site", None, "sec", None, None)
    blocks = P("site", "sec", None, None)
    return jax.shard_map(
        per_device,
        mesh=mesh,
        in_specs=(tensor, tensor, tensor, blocks, blocks, blocks,
                  P("site", None, None), P("site", None), P("site")),
        out_specs=(tensor, tensor),
        check_vma=False,
    )
```

```python
import functools

import jax
import jax.numpy as jnp
from jax import lax
from jax.experimental import pallas as pl
from jax.experimental.pallas import tpu as pltpu
from jax.sharding import PartitionSpec as P

NSI = 10
NAPP = 2
UNROLL = 8
VMEM_BYTES = 67043328
RESERVED = 10240 * 1024
SLACK = 44 * 1024
MESH = pl.DeviceIdType.MESH
F32 = jnp.float32
BF16 = jnp.bfloat16


def dot(a, b):
    return lax.dot_general(a, b, (((1,), (0,)), ((), ())), preferred_element_type=F32)


def dot_nt(a, b):
    return lax.dot_general(a, b, (((1,), (1,)), ((), ())), preferred_element_type=F32)


def dot_tn(a, b):
    return lax.dot_general(a, b, (((0,), (0,)), ((), ())), preferred_element_type=F32)


def split(x):
    hi = x.astype(BF16)
    return hi, (x - hi.astype(F32)).astype(BF16)


def beside(pair):
    return jnp.concatenate(pair, axis=1)


def below(pair):
    return jnp.concatenate(pair, axis=0)


def twice_wide(x):
    return beside((x, x))


def twice_tall(x):
    return below((x, x))


def kernel(
    steps, sites, parts, phys, owned,
    lc_in, rc_in, cs_in, cb_in, lseed_in, rseed_in, src_in, onsite_in, shift_in,
    *refs,
):
    blocks = phys * owned
    left_new, right_new = refs[:blocks], refs[blocks : 2 * blocks]
    (
    lc, rc, cs, cb, lseed, rseed, src, onsite, shift, site, fall,
    hold_l, lrecv, lsend, rrecv, psend, terms, lct, bond, ys, zs, env_r,
    gsend, grecv, usend, urecv, tns, tnr, trs, trr,
    s_in, s_ls, s_lr, s_ps, s_pr, s_gs, s_gr, s_us, s_ur, s_tns, s_tnr, s_trs, s_trr,
    ) = refs[2 * blocks :]
    j = lax.axis_index("site")
    me = lax.axis_index("sec")
    after, before = lax.rem(j + 1, sites), lax.rem(j + sites - 1, sites)
    off = me * owned
    width = lc.shape[-1]
    sectors = parts * owned
    pairs = sectors // 2

    def load(i, a, b):
        return pltpu.make_async_copy(a, b, s_in.at[i])

    loads = [
        load(0, lseed_in, lseed), load(1, rseed_in, rseed), load(2, rc_in, rc),
        load(3, lc_in, lc), load(4, cb_in, cb), load(5, cs_in, cs),
        load(6, src_in, src), load(7, onsite_in, onsite), load(8, shift_in, shift),
    ]
    for c in loads:
        c.start()

    def sec(d):
        return lax.rem(me + d, parts)

    def copy(a, b, ss, rs, to_site, to_sec):
        return pltpu.make_async_remote_copy(
            src_ref=a, dst_ref=b, send_sem=ss, recv_sem=rs,
            device_id={"site": to_site, "sec": to_sec}, device_id_type=MESH,
        )

    def c_seed(d):
        return copy(lseed.at[0], lrecv.at[0, me], s_ls.at[steps, d, 0], s_lr.at[0, me, 0], j, sec(d))

    def c_left(t, d, k):
        return copy(
            lsend.at[t, k], lrecv.at[t + 1, me, k], s_ls.at[t, d, k], s_lr.at[t + 1, me, k], after, sec(d)
        )

    def c_right(t, d):
        return copy(psend.at[t, d], rrecv.at[t, me], s_ps.at[t, d], s_pr.at[t, me], before, sec(d))

    def c_tn(d):
        return copy(tns, tnr.at[me], s_tns.at[d], s_tnr.at[me], j, sec(d))

    def c_tr(d):
        return copy(trs, trr.at[me], s_trs.at[d], s_trr.at[me], before, sec(d))

    def c_gram(d, p):
        return copy(gsend.at[p], grecv.at[me, p], s_gs.at[d, p], s_gr.at[me, p], j, sec(d))

    def c_unit(d):
        return copy(usend, urecv.at[me], s_us.at[d], s_ur.at[me], after, sec(d))

    def got(ref, sem):
        copy(ref, ref, s_us.at[0], sem, after, me).wait_recv()

    def c_out(side, s, k):
        a, b = (right_new, right_out) if side else (left_new, left_out)
        return pltpu.make_async_copy(a.at[0, s, k], b.at[0, s, k], s_out.at[side, s, k])

    barrier = pltpu.get_barrier_semaphore()
    for d in range(parts):
        for where in (after, before) if d == 0 else (after, before, j):
            pl.semaphore_signal(
                barrier, inc=1, device_id={"site": where, "sec": sec(d)}, device_id_type=MESH
            )
    loads[0].wait()
    pl.semaphore_wait(barrier, 3 * parts - 1)
    for d in range(1, parts):
        c_seed(d).start()

    for c in loads[6:]:
        c.wait()
    sources = [[src[0, s, off + k] for k in range(owned)] for s in range(phys)]

    def gathered(target):
        total = None
        for s in range(phys):
            hit, at = jnp.int32(0), jnp.int32(0)
            for k in range(owned):
                same = (sources[s][k] == target).astype(jnp.int32)
                hit, at = hit + same, at + same * k
            term = terms[s * owned + at] * hit.astype(F32)
            total = term if total is None else total + term
        return total

    rows = lax.broadcasted_iota(jnp.int32, (width, width), 0)
    cols = lax.broadcasted_iota(jnp.int32, (width, width), 1)
    diagonal = (rows == cols).astype(F32)
    half_diagonal = 0.5 * diagonal

    def traces(blocks):
        total = None
        for block in blocks:
            total = block.astype(F32) if total is None else total + block.astype(F32)
        return jnp.sum((total * diagonal).reshape(width // 8, 8, width), axis=0)

    loads[1].wait()
    for k in range(owned):
        env_r[k] = rseed[0, k]
    loads[2].wait()

    def seed_arrival():
        for k in range(owned):
            hold_l[off + k] = lseed[0, k]
        for d in range(1, parts):
            a = sec(d)
            got(lrecv.at[0, a], s_lr.at[0, a, 0])
            for k in range(owned):
                hold_l[a * owned + k] = lrecv[0, a, k]

    def left_arrival(t):
        for d in range(parts):
            a = sec(d)
            for k in range(owned):
                got(lrecv.at[t, a, k], s_lr.at[t, a, k])
                hold_l[a * owned + k] = lrecv[t, a, k]

    def right_arrival(t):
        for d in range(parts):
            a = sec(d)
            got(rrecv.at[t, a], s_pr.at[t, a])
        for k in range(owned):
            total = rrecv[t, 0, k].astype(F32)
            for a in range(1, parts):
                total = total + rrecv[t, a, k].astype(F32)
            env_r[k] = total.astype(BF16)

    def right_compute(t, last):
        for k in range(owned):
            stack = jnp.concatenate([rc[0, s, k] for s in range(phys)], axis=0)
            prod = dot(stack, env_r[k]).astype(BF16)
            for s in range(phys):
                terms[s * owned + k] = dot_nt(prod[s * width : (s + 1) * width], rc[0, s, k])
        for d in range(parts - 1, -1, -1):
            for i in range(owned):
                psend[t, d, i] = gathered(sec(d) * owned + i).astype(BF16)
            if not last:
                c_right(t, d).start()
        if last:
            trs[...] = traces([psend[t, d, i] for d in range(parts) for i in range(owned)])
            for d in range(parts - 1, -1, -1):
                c_tr(d).start()
            for d in range(parts - 1, -1, -1):
                c_right(t, d).start()

    def left_compute(t, last):
        prods = [
            [dot(hold_l[sources[s][k]], lc[0, s, k]).astype(BF16) for s in range(phys)]
            for k in range(owned)
        ]
        for k in range(owned):
            lsend[t, k] = dot(lct[k], below(prods[k])).astype(BF16)
            if last and k == owned - 1:
                tns[...] = traces([lsend[t, i] for i in range(owned)])
                for d in range(1, parts):
                    c_tn(d).start()
            for d in range(parts - 1, 0, -1):
                c_left(t, d, k).start()
        for k in range(owned):
            c_left(t, 0, k).start()

    right_compute(0, steps == 1)
    loads[3].wait()
    for k in range(owned):
        for s in range(phys):
            lct[k, :, s * width : (s + 1) * width] = lc[0, s, k].T
    seed_arrival()
    left_compute(0, steps == 1)

    def turn(t, carry):
        right_arrival(t - 1)
        right_compute(t, False)
        left_arrival(t)
        left_compute(t, False)
        return carry

    lax.fori_loop(1, steps - 1, turn, 0)
    if steps > 1:
        right_arrival(steps - 2)
        right_compute(steps - 1, True)
        left_arrival(steps - 1)
        left_compute(steps - 1, True)

    def scale_of(total):
        return (sectors * width) / jnp.sum(total, axis=(0, 1), keepdims=True)

    def begin(i, gram, block=None):
        norm = jnp.sqrt(jnp.sum(gram * gram, axis=(0, 1), keepdims=True))
        back, root = 1.0 / norm, 1.0 / jnp.sqrt(norm)
        hi, lo = split(gram)
        if block is None:
            square = dot(beside((hi, lo)), twice_tall(hi))
            first = gram * back
            ys[i] = 1.5 * first - 0.5 * ((square * back) * back)
            zs[i] = 1.5 * diagonal - 0.5 * first
        else:
            turned = block.T
            ys[i] = (1.5 * block.astype(F32) - 0.5 * (dot(block, hi) * back)) * root
            zs[i] = (1.5 * turned.astype(F32) - 0.5 * (dot(hi, turned) * back)) * root
        return root

    def deltas(these, swap=False):
        zh = [split(zs[i]) for i in these]
        yh = [split(ys[i]) for i in these]
        found = [
            (half_diagonal - 0.5 * (dot(y[0], z[0]) if swap else dot(z[0], y[0]))).astype(BF16)
            for z, y in zip(zh, yh)
        ]
        return zh, yh, found

    def advance(these):
        zh, yh, found = deltas(these)
        for i, z, y, delta in zip(these, zh, yh, found):
            ys[i] = ys[i] + dot(beside(y), twice_tall(delta))
            zs[i] = zs[i] + dot(twice_wide(delta), below(z))

    def loop(count, these):
        def body(n, carry):
            for again in range(UNROLL):
                advance(these)
            return carry

        lax.fori_loop(0, count // UNROLL, body, 0)
        for again in range(count % UNROLL):
            advance(these)

    bonds = list(range(owned))
    lefts = [owned + k for k in range(owned)]
    rights = [2 * owned + m for m in range(sectors)]

    right_arrival(steps - 1)
    for a in range(parts):
        got(trr.at[a], s_trr.at[a])
    total = trr[0]
    for a in range(1, parts):
        total = total + trr[a]
    scale = scale_of(total)
    for k in range(owned):
        env_r[k] = (env_r[k].astype(F32) * scale).astype(BF16)

    loads[4].wait()
    now = [cb[0, k] for k in range(owned)]

    def bond_product(k):
        return dot(dot(lsend[steps - 1, k], now[k]).astype(BF16), env_r[k])

    product = [bond_product(k) for k in range(owned)]
    loads[5].wait()

    left_arrival(steps)
    scale = scale_of(traces([hold_l[m] for m in range(sectors)]))
    states = [[cs[0, s, k] for s in range(phys)] for k in range(owned)]
    for repeat in range(NAPP):
        halves = [
            [dot(hold_l[sources[s][k]], states[k][s]).astype(BF16) for s in range(phys)]
            for k in range(owned)
        ]
        for k in range(owned):
            whole = dot(below(halves[k]), env_r[k]) * scale
            states[k] = [
                (whole[s * width : (s + 1) * width] + onsite[0, s] * states[k][s].astype(F32)).astype(BF16)
                for s in range(phys)
            ]
    for k in range(owned):
        site[k] = below(states[k])

    for k in range(owned):
        for s in range(phys):
            terms[s * owned + k] = dot_nt(states[k][s], states[k][s])
    for p in range(pairs):
        even, odd = gathered(2 * p), gathered(2 * p + 1)
        gsend[p, :width] = jnp.where(rows >= cols, even, odd)
        gsend[p, width:] = jnp.sum((odd * diagonal).reshape(width // 8, 8, width), axis=0)
        for d in range(1, parts):
            c_gram(d, p).start()

    total = tns[...]
    for d in range(1, parts):
        a = sec(d)
        got(tnr.at[a], s_tnr.at[a])
        total = total + tnr[a]
    bond_scale = scale_of(total)
    for repeat in range(NAPP):
        if repeat > 0:
            product = [bond_product(k) for k in range(owned)]
        for k in range(owned):
            now[k] = (product[k] * bond_scale + shift[0] * now[k].astype(F32)).astype(BF16)
    for k in range(owned):
        begin(bonds[k], dot_tn(now[k], now[k]), now[k])
    left_root = [
        begin(lefts[k], dot_tn(site[k], site[k])) for k in range(owned)
    ]
    loop(NSI - 2, bonds + lefts)
    advance(bonds)
    for k in range(owned):
        usend[k] = zs[k].astype(BF16)
    for d in range(parts - 1, -1, -1):
        c_unit(d).start()
    zh, yh, found = deltas(lefts)
    for k in range(owned):
        hi, lo = split(zs[k])
        wide = dot(beside(zh[k]), beside((twice_tall(hi), twice_tall(lo))))
        value = wide[:, :width] + wide[:, width:]
        factor = value + dot(twice_wide(found[k]), below(split(value)))
        whole = dot(site[k], (factor * left_root[k]).astype(BF16)).astype(BF16)
        for s in range(phys):
            left_new[s * owned + k][...] = whole[s * width : (s + 1) * width]

    packed = []
    for p in range(pairs):
        total, edge = gsend[p, :width], gsend[p, width:]
        for d in range(1, parts):
            a = sec(d)
            got(grecv.at[a, p], s_gr.at[a, p])
            total, edge = total + grecv[a, p, :width], edge + grecv[a, p, width:]
        packed.append((total, jnp.sum(edge, axis=0, keepdims=True)))
    right_root = []
    for p, (total, line) in enumerate(packed):
        turned = total.T
        right_root.append(begin(rights[2 * p], jnp.where(rows >= cols, total, turned)))
        odd = jnp.where(rows < cols, total, jnp.where(rows == cols, line, turned))
        right_root.append(begin(rights[2 * p + 1], odd))
    loop(NSI - 2, rights)
    for a in range(parts):
        got(urecv.at[a], s_ur.at[a])
    zh, yh, found = deltas(rights, swap=True)
    values = [
        dot(twice_wide(urecv[m // owned, m % owned]), below(zh[m])) for m in range(sectors)
    ]
    for m in range(sectors):
        factor = values[m] + dot(beside(split(values[m])), twice_tall(found[m]))
        fall[m] = (factor * right_root[m]).astype(BF16)
    for k in range(owned):
        for s in range(phys):
            block = site[k, s * width : (s + 1) * width]
            right_new[s * owned + k][...] = dot(fall[sources[s][k]], block).astype(BF16)

    def drain(t, carry):
        for d in range(parts):
            for k in range(owned):
                c_left(t, d, k).wait_send()
            c_right(t, d).wait_send()
        return carry

    lax.fori_loop(0, steps, drain, 0)
    for d in range(parts):
        c_tr(d).wait_send()
        c_unit(d).wait_send()
    for d in range(1, parts):
        c_seed(d).wait_send()
        c_tn(d).wait_send()
        for p in range(pairs):
            c_gram(d, p).wait_send()


def finish(phys, owned, *refs):
    blocks = phys * owned
    left_new, right_new, sems = refs[2 * blocks :]
    copies = []
    for i in range(2 * blocks):
        out = left_new if i < blocks else right_new
        s, k = (i % blocks) // owned, i % owned
        copies.append(pltpu.make_async_copy(refs[i], out.at[0, s, k], sems.at[i]))
        copies[-1].start()
    for c in copies:
        c.wait()


def per_device(lc, rc, cs, cb, lseed, rseed, src, onsite, shift):
    sites, parts = lax.axis_size("site"), lax.axis_size("sec")
    steps = sites // 4
    _, phys, owned, width, _ = lc.shape
    sectors = parts * owned
    pairs = sectors // 2
    block = (width, width)

    def vm(*shape, dtype=BF16):
        return pltpu.VMEM(shape, dtype)

    def dma(*shape):
        return pltpu.SemaphoreType.DMA(shape)

    in_hbm = pl.BlockSpec(memory_space=pltpu.HBM)
    in_vmem = pl.BlockSpec(memory_space=pltpu.VMEM)
    shape = jax.ShapeDtypeStruct(cs.shape, BF16)
    blocks = phys * owned
    room = VMEM_BYTES - RESERVED - 2 * cs.size * 2 - SLACK
    done = pl.pallas_call(
        functools.partial(kernel, steps, sites, parts, phys, owned),
        out_shape=[jax.ShapeDtypeStruct(block, BF16)] * (2 * blocks),
        in_specs=[in_hbm] * 9,
        out_specs=[in_vmem] * (2 * blocks),
        scratch_shapes=[
            vm(*lc.shape), vm(*rc.shape), vm(*cs.shape), vm(*cb.shape),
            vm(*lseed.shape), vm(*rseed.shape),
            pltpu.SMEM(src.shape, src.dtype), pltpu.SMEM(onsite.shape, F32), pltpu.SMEM(shift.shape, F32),
            vm(owned, phys * width, width), vm(sectors, *block),
            vm(sectors, *block),
            vm(steps + 1, parts, owned, *block),
            vm(steps, owned, *block),
            vm(steps, parts, owned, *block),
            vm(steps, parts, owned, *block),
            vm(phys * owned, *block, dtype=F32),
            vm(owned, width, phys * width),
            vm(owned, *block),
            vm(2 * owned + sectors, *block, dtype=F32),
            vm(2 * owned + sectors, *block, dtype=F32),
            vm(owned, *block),
            vm(pairs, width + 8, width, dtype=F32),
            vm(parts, pairs, width + 8, width, dtype=F32),
            vm(owned, *block),
            vm(parts, owned, *block),
            vm(8, width, dtype=F32),
            vm(parts, 8, width, dtype=F32),
            vm(8, width, dtype=F32),
            vm(parts, 8, width, dtype=F32),
            dma(9),
            dma(steps + 1, parts, owned), dma(steps + 1, parts, owned),
            dma(steps, parts), dma(steps, parts),
            dma(parts, pairs), dma(parts, pairs),
            dma(parts), dma(parts),
            dma(parts), dma(parts),
            dma(parts), dma(parts),
        ],
        compiler_params=pltpu.CompilerParams(
            collective_id=0, has_side_effects=True, vmem_limit_bytes=room
        ),
    )(lc, rc, cs, cb, lseed, rseed, src, onsite, shift)
    return pl.pallas_call(
        functools.partial(finish, phys, owned),
        out_shape=(shape, shape),
        in_specs=[in_vmem] * (2 * blocks),
        out_specs=(in_hbm, in_hbm),
        scratch_shapes=[dma(2 * blocks)],
        compiler_params=pltpu.CompilerParams(vmem_limit_bytes=8 * 1024 * 1024),
    )(*done)


def solution(mesh):
    tensor = P("site", None, "sec", None, None)
    blocks = P("site", "sec", None, None)
    return jax.shard_map(
        per_device,
        mesh=mesh,
        in_specs=(tensor, tensor, tensor, blocks, blocks, blocks,
                  P("site", None, None), P("site", None), P("site")),
        out_specs=(tensor, tensor),
        check_vma=False,
    )
```

```python
import functools

import jax
import jax.numpy as jnp
from jax import lax
from jax.experimental import pallas as pl
from jax.experimental.pallas import tpu as pltpu
from jax.sharding import PartitionSpec as P

NSI = 10
NAPP = 2
UNROLL = 8
VMEM_BYTES = 67043328
RESERVED = 10240 * 1024
SLACK = 44 * 1024
MESH = pl.DeviceIdType.MESH
F32 = jnp.float32
BF16 = jnp.bfloat16


def dot(a, b):
    return lax.dot_general(a, b, (((1,), (0,)), ((), ())), preferred_element_type=F32)


def dot_nt(a, b):
    return lax.dot_general(a, b, (((1,), (1,)), ((), ())), preferred_element_type=F32)


def dot_tn(a, b):
    return lax.dot_general(a, b, (((0,), (0,)), ((), ())), preferred_element_type=F32)


def split(x):
    hi = x.astype(BF16)
    return hi, (x - hi.astype(F32)).astype(BF16)


def beside(pair):
    return jnp.concatenate(pair, axis=1)


def below(pair):
    return jnp.concatenate(pair, axis=0)


def twice_wide(x):
    return beside((x, x))


def twice_tall(x):
    return below((x, x))


def kernel(
    steps, sites, parts, phys, owned,
    lc_in, rc_in, cs_in, cb_in, lseed_in, rseed_in, src_in, onsite_in, shift_in,
    *refs,
):
    left_new, right_new = refs[:phys], refs[phys : 2 * phys]
    lrecv = refs[2 * phys : 2 * phys + steps + 1]
    (
    lc, rc, cs, cb, lseed, rseed, src, onsite, shift, site, fall,
    lsend, rrecv, psend, terms, lct, bond, ys, zs, env_r,
    gsend, grecv, usend, urecv, tns, tnr, trs, trr,
    s_in, s_ls, s_lr, s_ps, s_pr, s_gs, s_gr, s_us, s_ur, s_tns, s_tnr, s_trs, s_trr,
    ) = refs[2 * phys + steps + 1 :]
    j = lax.axis_index("site")
    me = lax.axis_index("sec")
    after, before = lax.rem(j + 1, sites), lax.rem(j + sites - 1, sites)
    off = me * owned
    width = lc.shape[-1]
    sectors = parts * owned
    pairs = sectors // 2

    def load(i, a, b):
        return pltpu.make_async_copy(a, b, s_in.at[i])

    loads = [
        load(0, lseed_in, lseed), load(1, rseed_in, rseed), load(2, rc_in, rc),
        load(3, lc_in, lc), load(4, cb_in, cb), load(5, cs_in, cs),
        load(6, src_in, src), load(7, onsite_in, onsite), load(8, shift_in, shift),
    ]
    for c in loads:
        c.start()

    def sec(d):
        return lax.rem(me + d, parts)

    def copy(a, b, ss, rs, to_site, to_sec):
        return pltpu.make_async_remote_copy(
            src_ref=a, dst_ref=b, send_sem=ss, recv_sem=rs,
            device_id={"site": to_site, "sec": to_sec}, device_id_type=MESH,
        )

    def c_seed(d):
        return copy(lseed.at[0], lrecv[0].at[pl.ds(off, owned)], s_ls.at[steps, d, 0], s_lr.at[0, me, 0], j, sec(d))

    def c_left(t, d, k):
        return copy(
            lsend.at[t, k], lrecv[t + 1].at[off + k], s_ls.at[t, d, k], s_lr.at[t + 1, me, k], after, sec(d)
        )

    def c_right(t, d):
        return copy(psend.at[t, d], rrecv.at[t, me], s_ps.at[t, d], s_pr.at[t, me], before, sec(d))

    def c_tn(d):
        return copy(tns, tnr.at[me], s_tns.at[d], s_tnr.at[me], j, sec(d))

    def c_tr(d):
        return copy(trs, trr.at[me], s_trs.at[d], s_trr.at[me], before, sec(d))

    def c_gram(d, p):
        return copy(gsend.at[p], grecv.at[me, p], s_gs.at[d, p], s_gr.at[me, p], j, sec(d))

    def c_unit(d):
        return copy(usend, urecv.at[me], s_us.at[d], s_ur.at[me], after, sec(d))

    def got(ref, sem):
        copy(ref, ref, s_us.at[0], sem, after, me).wait_recv()

    def c_out(side, s, k):
        a, b = (right_new, right_out) if side else (left_new, left_out)
        return pltpu.make_async_copy(a.at[0, s, k], b.at[0, s, k], s_out.at[side, s, k])

    barrier = pltpu.get_barrier_semaphore()
    for d in range(parts):
        for where in (after, before) if d == 0 else (after, before, j):
            pl.semaphore_signal(
                barrier, inc=1, device_id={"site": where, "sec": sec(d)}, device_id_type=MESH
            )
    loads[0].wait()
    pl.semaphore_wait(barrier, 3 * parts - 1)
    for d in range(1, parts):
        c_seed(d).start()

    for c in loads[6:]:
        c.wait()
    sources = [[src[0, s, off + k] for k in range(owned)] for s in range(phys)]

    def gathered(target):
        total = None
        for s in range(phys):
            hit, at = jnp.int32(0), jnp.int32(0)
            for k in range(owned):
                same = (sources[s][k] == target).astype(jnp.int32)
                hit, at = hit + same, at + same * k
            term = terms[s * owned + at] * hit.astype(F32)
            total = term if total is None else total + term
        return total

    rows = lax.broadcasted_iota(jnp.int32, (width, width), 0)
    cols = lax.broadcasted_iota(jnp.int32, (width, width), 1)
    diagonal = (rows == cols).astype(F32)
    half_diagonal = 0.5 * diagonal

    def traces(blocks):
        total = None
        for block in blocks:
            total = block.astype(F32) if total is None else total + block.astype(F32)
        return jnp.sum((total * diagonal).reshape(width // 8, 8, width), axis=0)

    loads[1].wait()
    for k in range(owned):
        env_r[k] = rseed[0, k]
    loads[2].wait()

    def seed_arrival():
        for k in range(owned):
            lrecv[0][off + k] = lseed[0, k]
        for d in range(1, parts):
            a = sec(d)
            got(lrecv[0].at[pl.ds(a * owned, owned)], s_lr.at[0, a, 0])

    def left_arrival(t):
        for d in range(parts):
            a = sec(d)
            for k in range(owned):
                got(lrecv[t].at[a * owned + k], s_lr.at[t, a, k])

    def right_arrival(t):
        for d in range(parts):
            a = sec(d)
            got(rrecv.at[t, a], s_pr.at[t, a])
        for k in range(owned):
            total = rrecv[t, 0, k].astype(F32)
            for a in range(1, parts):
                total = total + rrecv[t, a, k].astype(F32)
            env_r[k] = total.astype(BF16)

    def right_compute(t, last):
        for k in range(owned):
            stack = jnp.concatenate([rc[0, s, k] for s in range(phys)], axis=0)
            prod = dot(stack, env_r[k]).astype(BF16)
            for s in range(phys):
                terms[s * owned + k] = dot_nt(prod[s * width : (s + 1) * width], rc[0, s, k])
        for d in range(parts - 1, -1, -1):
            for i in range(owned):
                psend[t, d, i] = gathered(sec(d) * owned + i).astype(BF16)
            if not last:
                c_right(t, d).start()
        if last:
            trs[...] = traces([psend[t, d, i] for d in range(parts) for i in range(owned)])
            for d in range(parts - 1, -1, -1):
                c_tr(d).start()
            for d in range(parts - 1, -1, -1):
                c_right(t, d).start()

    def left_compute(t, last):
        prods = [
            [dot(lrecv[t][sources[s][k]], lc[0, s, k]).astype(BF16) for s in range(phys)]
            for k in range(owned)
        ]
        for k in range(owned):
            lsend[t, k] = dot(lct[k], below(prods[k])).astype(BF16)
            if last and k == owned - 1:
                tns[...] = traces([lsend[t, i] for i in range(owned)])
                for d in range(1, parts):
                    c_tn(d).start()
            for d in range(parts - 1, 0, -1):
                c_left(t, d, k).start()
        for k in range(owned):
            c_left(t, 0, k).start()

    right_compute(0, steps == 1)
    loads[3].wait()
    for k in range(owned):
        for s in range(phys):
            lct[k, :, s * width : (s + 1) * width] = lc[0, s, k].T
    seed_arrival()
    left_compute(0, steps == 1)

    for t in range(1, steps):
        right_arrival(t - 1)
        right_compute(t, t == steps - 1)
        left_arrival(t)
        left_compute(t, t == steps - 1)

    def scale_of(total):
        return (sectors * width) / jnp.sum(total, axis=(0, 1), keepdims=True)

    def begin(i, gram, block=None):
        norm = jnp.sqrt(jnp.sum(gram * gram, axis=(0, 1), keepdims=True))
        back, root = 1.0 / norm, 1.0 / jnp.sqrt(norm)
        hi, lo = split(gram)
        if block is None:
            square = dot(beside((hi, lo)), twice_tall(hi))
            first = gram * back
            ys[i] = 1.5 * first - 0.5 * ((square * back) * back)
            zs[i] = 1.5 * diagonal - 0.5 * first
        else:
            turned = block.T
            ys[i] = (1.5 * block.astype(F32) - 0.5 * (dot(block, hi) * back)) * root
            zs[i] = (1.5 * turned.astype(F32) - 0.5 * (dot(hi, turned) * back)) * root
        return root

    def deltas(these, swap=False):
        zh = [split(zs[i]) for i in these]
        yh = [split(ys[i]) for i in these]
        found = [
            (half_diagonal - 0.5 * (dot(y[0], z[0]) if swap else dot(z[0], y[0]))).astype(BF16)
            for z, y in zip(zh, yh)
        ]
        return zh, yh, found

    def advance(these):
        zh, yh, found = deltas(these)
        for i, z, y, delta in zip(these, zh, yh, found):
            ys[i] = ys[i] + dot(beside(y), twice_tall(delta))
            zs[i] = zs[i] + dot(twice_wide(delta), below(z))

    def loop(count, these):
        def body(n, carry):
            for again in range(UNROLL):
                advance(these)
            return carry

        lax.fori_loop(0, count // UNROLL, body, 0)
        for again in range(count % UNROLL):
            advance(these)

    bonds = list(range(owned))
    lefts = [owned + k for k in range(owned)]
    rights = [2 * owned + m for m in range(sectors)]

    right_arrival(steps - 1)
    for a in range(parts):
        got(trr.at[a], s_trr.at[a])
    total = trr[0]
    for a in range(1, parts):
        total = total + trr[a]
    scale = scale_of(total)
    for k in range(owned):
        env_r[k] = (env_r[k].astype(F32) * scale).astype(BF16)

    loads[4].wait()
    now = [cb[0, k] for k in range(owned)]

    def bond_product(k):
        return dot(dot(lsend[steps - 1, k], now[k]).astype(BF16), env_r[k])

    product = [bond_product(k) for k in range(owned)]
    loads[5].wait()

    left_arrival(steps)
    scale = scale_of(traces([lrecv[steps][m] for m in range(sectors)]))
    states = [[cs[0, s, k] for s in range(phys)] for k in range(owned)]
    for repeat in range(NAPP):
        halves = [
            [dot(lrecv[steps][sources[s][k]], states[k][s]).astype(BF16) for s in range(phys)]
            for k in range(owned)
        ]
        for k in range(owned):
            whole = dot(below(halves[k]), env_r[k]) * scale
            states[k] = [
                (whole[s * width : (s + 1) * width] + onsite[0, s] * states[k][s].astype(F32)).astype(BF16)
                for s in range(phys)
            ]
    for k in range(owned):
        site[k] = below(states[k])

    for k in range(owned):
        for s in range(phys):
            terms[s * owned + k] = dot_nt(states[k][s], states[k][s])
    for p in range(pairs):
        even, odd = gathered(2 * p), gathered(2 * p + 1)
        gsend[p, :width] = jnp.where(rows >= cols, even, odd)
        gsend[p, width:] = jnp.sum((odd * diagonal).reshape(width // 8, 8, width), axis=0)
        for d in range(1, parts):
            c_gram(d, p).start()

    total = tns[...]
    for d in range(1, parts):
        a = sec(d)
        got(tnr.at[a], s_tnr.at[a])
        total = total + tnr[a]
    bond_scale = scale_of(total)
    for repeat in range(NAPP):
        if repeat > 0:
            product = [bond_product(k) for k in range(owned)]
        for k in range(owned):
            now[k] = (product[k] * bond_scale + shift[0] * now[k].astype(F32)).astype(BF16)
    for k in range(owned):
        begin(bonds[k], dot_tn(now[k], now[k]), now[k])
    left_root = [
        begin(lefts[k], dot_tn(site[k], site[k])) for k in range(owned)
    ]
    advance(bonds)
    loop(NSI - 2, bonds + lefts)
    for k in range(owned):
        usend[k] = zs[k].astype(BF16)
    for d in range(parts - 1, -1, -1):
        c_unit(d).start()
    zh, yh, found = deltas(lefts)
    for k in range(owned):
        hi, lo = split(zs[k])
        wide = dot(beside(zh[k]), beside((twice_tall(hi), twice_tall(lo))))
        value = wide[:, :width] + wide[:, width:]
        factor = value + dot(twice_wide(found[k]), below(split(value)))
        whole = dot(site[k], (factor * left_root[k]).astype(BF16)).astype(BF16)
        for s in range(phys):
            left_new[s][k] = whole[s * width : (s + 1) * width]

    for t in range(steps):
        for d in range(parts):
            for k in range(owned):
                c_left(t, d, k).wait_send()
            c_right(t, d).wait_send()
    for d in range(parts):
        c_tr(d).wait_send()
    for d in range(1, parts):
        c_seed(d).wait_send()
        c_tn(d).wait_send()
    packed = []
    for p in range(pairs):
        total, edge = gsend[p, :width], gsend[p, width:]
        for d in range(1, parts):
            a = sec(d)
            got(grecv.at[a, p], s_gr.at[a, p])
            total, edge = total + grecv[a, p, :width], edge + grecv[a, p, width:]
        packed.append((total, jnp.sum(edge, axis=0, keepdims=True)))
    right_root = []
    for p, (total, line) in enumerate(packed):
        turned = total.T
        right_root.append(begin(rights[2 * p], jnp.where(rows >= cols, total, turned)))
        odd = jnp.where(rows < cols, total, jnp.where(rows == cols, line, turned))
        right_root.append(begin(rights[2 * p + 1], odd))
    loop(NSI - 2, rights)
    for a in range(parts):
        got(urecv.at[a], s_ur.at[a])
    zh, yh, found = deltas(rights, swap=True)
    values = [
        dot(twice_wide(urecv[m // owned, m % owned]), below(zh[m])) for m in range(sectors)
    ]
    for m in range(sectors):
        factor = values[m] + dot(beside(split(values[m])), twice_tall(found[m]))
        fall[m] = (factor * right_root[m]).astype(BF16)
    for k in range(owned):
        for s in range(phys):
            block = site[k, s * width : (s + 1) * width]
            right_new[s][k] = dot(fall[sources[s][k]], block).astype(BF16)

    for d in range(parts):
        c_unit(d).wait_send()
    for d in range(1, parts):
        for p in range(pairs):
            c_gram(d, p).wait_send()


def finish(phys, *refs):
    left_new, right_new, sems = refs[2 * phys :]
    copies = []
    for i in range(2 * phys):
        out = left_new if i < phys else right_new
        copies.append(pltpu.make_async_copy(refs[i], out.at[0, i % phys], sems.at[i]))
        copies[-1].start()
    for c in copies:
        c.wait()


def per_device(lc, rc, cs, cb, lseed, rseed, src, onsite, shift):
    sites, parts = lax.axis_size("site"), lax.axis_size("sec")
    steps = sites // 4
    _, phys, owned, width, _ = lc.shape
    sectors = parts * owned
    pairs = sectors // 2
    block = (width, width)

    def vm(*shape, dtype=BF16):
        return pltpu.VMEM(shape, dtype)

    def dma(*shape):
        return pltpu.SemaphoreType.DMA(shape)

    in_hbm = pl.BlockSpec(memory_space=pltpu.HBM)
    in_vmem = pl.BlockSpec(memory_space=pltpu.VMEM)
    shape = jax.ShapeDtypeStruct(cs.shape, BF16)
    room = VMEM_BYTES - RESERVED - 2 * cs.size * 2 - SLACK
    done = pl.pallas_call(
        functools.partial(kernel, steps, sites, parts, phys, owned),
        out_shape=[jax.ShapeDtypeStruct((owned, *block), BF16)] * (2 * phys),
        in_specs=[in_hbm] * 9,
        out_specs=[in_vmem] * (2 * phys),
        scratch_shapes=[vm(sectors, *block)] * (steps + 1) + [
            vm(*lc.shape), vm(*rc.shape), vm(*cs.shape), vm(*cb.shape),
            vm(*lseed.shape), vm(*rseed.shape),
            pltpu.SMEM(src.shape, src.dtype), pltpu.SMEM(onsite.shape, F32), pltpu.SMEM(shift.shape, F32),
            vm(owned, phys * width, width), vm(sectors, *block),
            vm(steps, owned, *block),
            vm(steps, parts, owned, *block),
            vm(steps, parts, owned, *block),
            vm(phys * owned, *block, dtype=F32),
            vm(owned, width, phys * width),
            vm(owned, *block),
            vm(2 * owned + sectors, *block, dtype=F32),
            vm(2 * owned + sectors, *block, dtype=F32),
            vm(owned, *block),
            vm(pairs, width + 8, width, dtype=F32),
            vm(parts, pairs, width + 8, width, dtype=F32),
            vm(owned, *block),
            vm(parts, owned, *block),
            vm(8, width, dtype=F32),
            vm(parts, 8, width, dtype=F32),
            vm(8, width, dtype=F32),
            vm(parts, 8, width, dtype=F32),
            dma(9),
            dma(steps + 1, parts, owned), dma(steps + 1, parts, owned),
            dma(steps, parts), dma(steps, parts),
            dma(parts, pairs), dma(parts, pairs),
            dma(parts), dma(parts),
            dma(parts), dma(parts),
            dma(parts), dma(parts),
        ],
        compiler_params=pltpu.CompilerParams(
            collective_id=0, has_side_effects=True, vmem_limit_bytes=room
        ),
    )(lc, rc, cs, cb, lseed, rseed, src, onsite, shift)
    return pl.pallas_call(
        functools.partial(finish, phys),
        out_shape=(shape, shape),
        in_specs=[in_vmem] * (2 * phys),
        out_specs=(in_hbm, in_hbm),
        scratch_shapes=[dma(2 * phys)],
        compiler_params=pltpu.CompilerParams(vmem_limit_bytes=8 * 1024 * 1024),
    )(*done)


def solution(mesh):
    tensor = P("site", None, "sec", None, None)
    blocks = P("site", "sec", None, None)
    return jax.shard_map(
        per_device,
        mesh=mesh,
        in_specs=(tensor, tensor, tensor, blocks, blocks, blocks,
                  P("site", None, None), P("site", None), P("site")),
        out_specs=(tensor, tensor),
        check_vma=False,
    )
```

```python
import functools

import jax
import jax.numpy as jnp
from jax import lax
from jax.experimental import pallas as pl
from jax.experimental.pallas import tpu as pltpu
from jax.sharding import PartitionSpec as P

NSI = 10
NAPP = 2
UNROLL = 8
VMEM_BYTES = 67043328
RESERVED = 10240 * 1024
SLACK = 44 * 1024
MESH = pl.DeviceIdType.MESH
F32 = jnp.float32
BF16 = jnp.bfloat16


def dot(a, b):
    return lax.dot_general(a, b, (((1,), (0,)), ((), ())), preferred_element_type=F32)


def dot_nt(a, b):
    return lax.dot_general(a, b, (((1,), (1,)), ((), ())), preferred_element_type=F32)


def dot_tn(a, b):
    return lax.dot_general(a, b, (((0,), (0,)), ((), ())), preferred_element_type=F32)


def split(x):
    hi = x.astype(BF16)
    return hi, (x - hi.astype(F32)).astype(BF16)


def beside(pair):
    return jnp.concatenate(pair, axis=1)


def below(pair):
    return jnp.concatenate(pair, axis=0)


def twice_wide(x):
    return beside((x, x))


def twice_tall(x):
    return below((x, x))


def kernel(
    steps, sites, parts, phys, owned,
    lc_in, rc_in, cs_in, cb_in, lseed_in, rseed_in, src_in, onsite_in, shift_in,
    *refs,
):
    left_new, right_new = refs[:phys], refs[phys : 2 * phys]
    lrecv = refs[2 * phys : 2 * phys + steps + 1]
    (
    lc, rc, cs, cb, lseed, rseed, src, onsite, shift, site, fall,
    ahead, lsend, rrecv, psend, terms, lct, bond, ys, zs, env_r,
    gsend, grecv, usend, urecv, tns, tnr, trs, trr,
    s_in, s_ls, s_lr, s_ps, s_pr, s_gs, s_gr, s_us, s_ur, s_tns, s_tnr, s_trs, s_trr,
    ) = refs[2 * phys + steps + 1 :]
    j = lax.axis_index("site")
    me = lax.axis_index("sec")
    after, before = lax.rem(j + 1, sites), lax.rem(j + sites - 1, sites)
    off = me * owned
    width = lc.shape[-1]
    sectors = parts * owned
    pairs = sectors // 2

    def load(i, a, b):
        return pltpu.make_async_copy(a, b, s_in.at[i])

    loads = [
        load(0, lseed_in, lseed), load(1, rseed_in, rseed), load(2, rc_in, rc),
        load(3, lc_in, lc), load(4, cb_in, cb), load(5, cs_in, cs),
        load(6, src_in, src), load(7, onsite_in, onsite), load(8, shift_in, shift),
    ]
    for c in loads:
        c.start()

    def sec(d):
        return lax.rem(me + d, parts)

    def copy(a, b, ss, rs, to_site, to_sec):
        return pltpu.make_async_remote_copy(
            src_ref=a, dst_ref=b, send_sem=ss, recv_sem=rs,
            device_id={"site": to_site, "sec": to_sec}, device_id_type=MESH,
        )

    def c_seed(d):
        return copy(lseed.at[0], lrecv[0].at[pl.ds(off, owned)], s_ls.at[steps, d, 0], s_lr.at[0, me, 0], j, sec(d))

    def c_left(t, d, k):
        return copy(
            lsend.at[t, k], lrecv[t + 1].at[off + k], s_ls.at[t, d, k], s_lr.at[t + 1, me, k], after, sec(d)
        )

    def c_right(t, d):
        return copy(psend.at[t, d], rrecv.at[t, me], s_ps.at[t, d], s_pr.at[t, me], before, sec(d))

    def c_tn(d):
        return copy(tns, tnr.at[me], s_tns.at[d], s_tnr.at[me], j, sec(d))

    def c_tr(d):
        return copy(trs, trr.at[me], s_trs.at[d], s_trr.at[me], before, sec(d))

    def c_gram(d, p):
        return copy(gsend.at[p], grecv.at[me, p], s_gs.at[d, p], s_gr.at[me, p], j, sec(d))

    def c_unit(d):
        return copy(usend, urecv.at[me], s_us.at[d], s_ur.at[me], after, sec(d))

    def got(ref, sem):
        copy(ref, ref, s_us.at[0], sem, after, me).wait_recv()

    def c_out(side, s, k):
        a, b = (right_new, right_out) if side else (left_new, left_out)
        return pltpu.make_async_copy(a.at[0, s, k], b.at[0, s, k], s_out.at[side, s, k])

    barrier = pltpu.get_barrier_semaphore()
    for d in range(parts):
        for where in (after, before) if d == 0 else (after, before, j):
            pl.semaphore_signal(
                barrier, inc=1, device_id={"site": where, "sec": sec(d)}, device_id_type=MESH
            )
    loads[0].wait()
    pl.semaphore_wait(barrier, 3 * parts - 1)
    for d in range(1, parts):
        c_seed(d).start()

    for c in loads[6:]:
        c.wait()
    sources = [[src[0, s, off + k] for k in range(owned)] for s in range(phys)]

    def gathered(target):
        total = None
        for s in range(phys):
            hit, at = jnp.int32(0), jnp.int32(0)
            for k in range(owned):
                same = (sources[s][k] == target).astype(jnp.int32)
                hit, at = hit + same, at + same * k
            term = terms[s * owned + at] * hit.astype(F32)
            total = term if total is None else total + term
        return total

    rows = lax.broadcasted_iota(jnp.int32, (width, width), 0)
    cols = lax.broadcasted_iota(jnp.int32, (width, width), 1)
    diagonal = (rows == cols).astype(F32)
    half_diagonal = 0.5 * diagonal

    def traces(blocks):
        total = None
        for block in blocks:
            total = block.astype(F32) if total is None else total + block.astype(F32)
        return jnp.sum((total * diagonal).reshape(width // 8, 8, width), axis=0)

    loads[1].wait()
    for k in range(owned):
        env_r[k] = rseed[0, k]
    loads[2].wait()

    def seed_arrival():
        for k in range(owned):
            lrecv[0][off + k] = lseed[0, k]
        for d in range(1, parts):
            a = sec(d)
            got(lrecv[0].at[pl.ds(a * owned, owned)], s_lr.at[0, a, 0])

    def left_arrival(t):
        for d in range(parts):
            a = sec(d)
            for k in range(owned):
                got(lrecv[t].at[a * owned + k], s_lr.at[t, a, k])

    def right_arrival(t):
        for d in range(parts):
            a = sec(d)
            got(rrecv.at[t, a], s_pr.at[t, a])
        for k in range(owned):
            total = rrecv[t, 0, k].astype(F32)
            for a in range(1, parts):
                total = total + rrecv[t, a, k].astype(F32)
            env_r[k] = total.astype(BF16)

    def right_compute(t, last):
        for k in range(owned):
            stack = jnp.concatenate([rc[0, s, k] for s in range(phys)], axis=0)
            prod = dot(stack, env_r[k]).astype(BF16)
            for s in range(phys):
                terms[s * owned + k] = dot_nt(prod[s * width : (s + 1) * width], rc[0, s, k])
        for d in range(parts - 1, -1, -1):
            for i in range(owned):
                psend[t, d, i] = gathered(sec(d) * owned + i).astype(BF16)
            if not last:
                c_right(t, d).start()
        if last:
            trs[...] = traces([psend[t, d, i] for d in range(parts) for i in range(owned)])
            for d in range(parts - 1, -1, -1):
                c_tr(d).start()
            for d in range(parts - 1, -1, -1):
                c_right(t, d).start()

    def left_compute(t, last):
        prods = [
            [dot(lrecv[t][sources[s][k]], lc[0, s, k]).astype(BF16) for s in range(phys)]
            for k in range(owned)
        ]
        for k in range(owned):
            lsend[t, k] = dot(lct[k], below(prods[k])).astype(BF16)
            if last and k == owned - 1:
                tns[...] = traces([lsend[t, i] for i in range(owned)])
                for d in range(1, parts):
                    c_tn(d).start()
            for d in range(parts - 1, 0, -1):
                c_left(t, d, k).start()
        for k in range(owned):
            c_left(t, 0, k).start()

    right_compute(0, steps == 1)
    loads[3].wait()
    for k in range(owned):
        for s in range(phys):
            lct[k, :, s * width : (s + 1) * width] = lc[0, s, k].T
    seed_arrival()
    left_compute(0, steps == 1)

    for t in range(1, steps):
        right_arrival(t - 1)
        right_compute(t, t == steps - 1)
        left_arrival(t)
        left_compute(t, t == steps - 1)

    def scale_of(total):
        return (sectors * width) / jnp.sum(total, axis=(0, 1), keepdims=True)

    def begin(i, gram, block=None):
        norm = jnp.sqrt(jnp.sum(gram * gram, axis=(0, 1), keepdims=True))
        back, root = 1.0 / norm, 1.0 / jnp.sqrt(norm)
        hi, lo = split(gram)
        if block is None:
            square = dot(beside((hi, lo)), twice_tall(hi))
            first = gram * back
            ys[i] = 1.5 * first - 0.5 * ((square * back) * back)
            zs[i] = 1.5 * diagonal - 0.5 * first
        else:
            turned = block.T
            ys[i] = (1.5 * block.astype(F32) - 0.5 * (dot(block, hi) * back)) * root
            zs[i] = (1.5 * turned.astype(F32) - 0.5 * (dot(hi, turned) * back)) * root
        return root

    def deltas(these, swap=False):
        zh = [split(zs[i]) for i in these]
        yh = [split(ys[i]) for i in these]
        found = [
            (half_diagonal - 0.5 * (dot(y[0], z[0]) if swap else dot(z[0], y[0]))).astype(BF16)
            for z, y in zip(zh, yh)
        ]
        return zh, yh, found

    def advance(these):
        zh, yh, found = deltas(these)
        for i, z, y, delta in zip(these, zh, yh, found):
            ys[i] = ys[i] + dot(beside(y), twice_tall(delta))
            zs[i] = zs[i] + dot(twice_wide(delta), below(z))

    def loop(count, these):
        def body(n, carry):
            for again in range(UNROLL):
                advance(these)
            return carry

        lax.fori_loop(0, count // UNROLL, body, 0)
        for again in range(count % UNROLL):
            advance(these)

    bonds = list(range(owned))
    lefts = [owned + k for k in range(owned)]
    rights = [2 * owned + m for m in range(sectors)]

    right_arrival(steps - 1)
    for a in range(parts):
        got(trr.at[a], s_trr.at[a])
    total = trr[0]
    for a in range(1, parts):
        total = total + trr[a]
    scale = scale_of(total)
    for k in range(owned):
        env_r[k] = (env_r[k].astype(F32) * scale).astype(BF16)

    loads[4].wait()
    now = [cb[0, k] for k in range(owned)]

    def bond_product(k):
        return dot(dot(lsend[steps - 1, k], now[k]).astype(BF16), env_r[k])

    product = [bond_product(k) for k in range(owned)]
    loads[5].wait()
    for k in range(owned):
        ahead[k] = dot(below([cs[0, s, k] for s in range(phys)]), env_r[k]).astype(BF16)

    left_arrival(steps)
    scale = scale_of(traces([lrecv[steps][m] for m in range(sectors)]))
    states = [[cs[0, s, k] for s in range(phys)] for k in range(owned)]
    for repeat in range(NAPP):
        if repeat == 0:
            wholes = [
                [
                    dot(lrecv[steps][sources[s][k]], ahead[k, s * width : (s + 1) * width])
                    for s in range(phys)
                ]
                for k in range(owned)
            ]
        else:
            halves = [
                [dot(lrecv[steps][sources[s][k]], states[k][s]).astype(BF16) for s in range(phys)]
                for k in range(owned)
            ]
            wholes = [dot(below(halves[k]), env_r[k]) for k in range(owned)]
            wholes = [
                [whole[s * width : (s + 1) * width] for s in range(phys)] for whole in wholes
            ]
        states = [
            [
                (wholes[k][s] * scale + onsite[0, s] * states[k][s].astype(F32)).astype(BF16)
                for s in range(phys)
            ]
            for k in range(owned)
        ]
    for k in range(owned):
        site[k] = below(states[k])

    for k in range(owned):
        for s in range(phys):
            terms[s * owned + k] = dot_nt(states[k][s], states[k][s])
    for p in range(pairs):
        even, odd = gathered(2 * p), gathered(2 * p + 1)
        gsend[p, :width] = jnp.where(rows >= cols, even, odd)
        gsend[p, width:] = jnp.sum((odd * diagonal).reshape(width // 8, 8, width), axis=0)
        for d in range(1, parts):
            c_gram(d, p).start()

    total = tns[...]
    for d in range(1, parts):
        a = sec(d)
        got(tnr.at[a], s_tnr.at[a])
        total = total + tnr[a]
    bond_scale = scale_of(total)
    for repeat in range(NAPP):
        if repeat > 0:
            product = [bond_product(k) for k in range(owned)]
        for k in range(owned):
            now[k] = (product[k] * bond_scale + shift[0] * now[k].astype(F32)).astype(BF16)
    for k in range(owned):
        begin(bonds[k], dot_tn(now[k], now[k]), now[k])
    left_root = [
        begin(lefts[k], dot_tn(site[k], site[k])) for k in range(owned)
    ]
    advance(bonds)
    loop(NSI - 2, bonds + lefts)
    for k in range(owned):
        usend[k] = zs[k].astype(BF16)
    for d in range(parts - 1, -1, -1):
        c_unit(d).start()
    zh, yh, found = deltas(lefts)
    for k in range(owned):
        hi, lo = split(zs[k])
        wide = dot(beside(zh[k]), beside((twice_tall(hi), twice_tall(lo))))
        value = wide[:, :width] + wide[:, width:]
        factor = value + dot(twice_wide(found[k]), below(split(value)))
        whole = dot(site[k], (factor * left_root[k]).astype(BF16)).astype(BF16)
        for s in range(phys):
            left_new[s][k] = whole[s * width : (s + 1) * width]

    for t in range(steps):
        for d in range(parts):
            for k in range(owned):
                c_left(t, d, k).wait_send()
            c_right(t, d).wait_send()
    for d in range(parts):
        c_tr(d).wait_send()
    for d in range(1, parts):
        c_seed(d).wait_send()
        c_tn(d).wait_send()
    packed = []
    for p in range(pairs):
        total, edge = gsend[p, :width], gsend[p, width:]
        for d in range(1, parts):
            a = sec(d)
            got(grecv.at[a, p], s_gr.at[a, p])
            total, edge = total + grecv[a, p, :width], edge + grecv[a, p, width:]
        packed.append((total, jnp.sum(edge, axis=0, keepdims=True)))
    right_root = []
    for p, (total, line) in enumerate(packed):
        turned = total.T
        right_root.append(begin(rights[2 * p], jnp.where(rows >= cols, total, turned)))
        odd = jnp.where(rows < cols, total, jnp.where(rows == cols, line, turned))
        right_root.append(begin(rights[2 * p + 1], odd))
    loop(NSI - 2, rights)
    for a in range(parts):
        got(urecv.at[a], s_ur.at[a])
    zh, yh, found = deltas(rights, swap=True)
    values = [
        dot(twice_wide(urecv[m // owned, m % owned]), below(zh[m])) for m in range(sectors)
    ]
    for m in range(sectors):
        factor = values[m] + dot(beside(split(values[m])), twice_tall(found[m]))
        fall[m] = (factor * right_root[m]).astype(BF16)
    for k in range(owned):
        for s in range(phys):
            block = site[k, s * width : (s + 1) * width]
            right_new[s][k] = dot(fall[sources[s][k]], block).astype(BF16)

    for d in range(parts):
        c_unit(d).wait_send()
    for d in range(1, parts):
        for p in range(pairs):
            c_gram(d, p).wait_send()


def finish(phys, *refs):
    left_new, right_new, sems = refs[2 * phys :]
    copies = []
    for i in range(2 * phys):
        out = left_new if i < phys else right_new
        copies.append(pltpu.make_async_copy(refs[i], out.at[0, i % phys], sems.at[i]))
        copies[-1].start()
    for c in copies:
        c.wait()


def per_device(lc, rc, cs, cb, lseed, rseed, src, onsite, shift):
    sites, parts = lax.axis_size("site"), lax.axis_size("sec")
    steps = sites // 4
    _, phys, owned, width, _ = lc.shape
    sectors = parts * owned
    pairs = sectors // 2
    block = (width, width)

    def vm(*shape, dtype=BF16):
        return pltpu.VMEM(shape, dtype)

    def dma(*shape):
        return pltpu.SemaphoreType.DMA(shape)

    in_hbm = pl.BlockSpec(memory_space=pltpu.HBM)
    in_vmem = pl.BlockSpec(memory_space=pltpu.VMEM)
    shape = jax.ShapeDtypeStruct(cs.shape, BF16)
    room = VMEM_BYTES - RESERVED - 2 * cs.size * 2 - SLACK
    done = pl.pallas_call(
        functools.partial(kernel, steps, sites, parts, phys, owned),
        out_shape=[jax.ShapeDtypeStruct((owned, *block), BF16)] * (2 * phys),
        in_specs=[in_hbm] * 9,
        out_specs=[in_vmem] * (2 * phys),
        scratch_shapes=[vm(sectors, *block)] * (steps + 1) + [
            vm(*lc.shape), vm(*rc.shape), vm(*cs.shape), vm(*cb.shape),
            vm(*lseed.shape), vm(*rseed.shape),
            pltpu.SMEM(src.shape, src.dtype), pltpu.SMEM(onsite.shape, F32), pltpu.SMEM(shift.shape, F32),
            vm(owned, phys * width, width), vm(sectors, *block),
            vm(owned, phys * width, width),
            vm(steps, owned, *block),
            vm(steps, parts, owned, *block),
            vm(steps, parts, owned, *block),
            vm(phys * owned, *block, dtype=F32),
            vm(owned, width, phys * width),
            vm(owned, *block),
            vm(2 * owned + sectors, *block, dtype=F32),
            vm(2 * owned + sectors, *block, dtype=F32),
            vm(owned, *block),
            vm(pairs, width + 8, width, dtype=F32),
            vm(parts, pairs, width + 8, width, dtype=F32),
            vm(owned, *block),
            vm(parts, owned, *block),
            vm(8, width, dtype=F32),
            vm(parts, 8, width, dtype=F32),
            vm(8, width, dtype=F32),
            vm(parts, 8, width, dtype=F32),
            dma(9),
            dma(steps + 1, parts, owned), dma(steps + 1, parts, owned),
            dma(steps, parts), dma(steps, parts),
            dma(parts, pairs), dma(parts, pairs),
            dma(parts), dma(parts),
            dma(parts), dma(parts),
            dma(parts), dma(parts),
        ],
        compiler_params=pltpu.CompilerParams(
            collective_id=0, has_side_effects=True, vmem_limit_bytes=room
        ),
    )(lc, rc, cs, cb, lseed, rseed, src, onsite, shift)
    return pl.pallas_call(
        functools.partial(finish, phys),
        out_shape=(shape, shape),
        in_specs=[in_vmem] * (2 * phys),
        out_specs=(in_hbm, in_hbm),
        scratch_shapes=[dma(2 * phys)],
        compiler_params=pltpu.CompilerParams(vmem_limit_bytes=8 * 1024 * 1024),
    )(*done)


def solution(mesh):
    tensor = P("site", None, "sec", None, None)
    blocks = P("site", "sec", None, None)
    return jax.shard_map(
        per_device,
        mesh=mesh,
        in_specs=(tensor, tensor, tensor, blocks, blocks, blocks,
                  P("site", None, None), P("site", None), P("site")),
        out_specs=(tensor, tensor),
        check_vma=False,
    )
```
